256 devices in a mesh: dp: 16 (over x_hi, z), param: 16 (over y, x_lo, core).
Axes of the slice: x: 4 (x_hi: 2, x_lo: 2; x = x_hi * 2 + x_lo), y: 4, z: 8, core: 2. Of those that a mesh axis runs over, the one named last changes fastest.
Arguments:
- ex_grads: bfloat16 [1536, 20480], P('dp', 'param'), may hold values from -6 to 6
- tgt_grads: bfloat16 [4096, 20480], P('dp', 'param'), may hold values from -6 to 6
- projection: bfloat16 [20480, 4096], P('param'), may hold values from -0.0390625 to 0.0390625
- example_weight: float32 [1536], P('param'), may hold values from 0.05 to 1
Outputs:
- scores: float32 [4096, 1536], P('dp', 'param')
The draws below stay inside these ranges and needn't reach their ends.
All inputs are finite; a program needn't handle non-finite values.
Results may differ from the reference program's by a relative error of at most 0.0078.
Values may be sent and summed in bfloat16 or wider, within the bound.
A program may use at most 192 MiB of HBM per device.

```python
import math
import jax
import jax.numpy as jnp

COLS = 4096
EXAMPLES = 1536
TARGETS = 4096
PARAMS = 20480


def latent_setup(key):
    count = min(48, COLS // 2, PARAMS // 2, EXAMPLES // 4)
    top_value = EXAMPLES / 4.0
    low_value = 3.0
    fraction = jnp.arange(count, dtype=jnp.float32) / (count - 1)
    eigen = top_value * jnp.power(jnp.float32(low_value / top_value), fraction)
    scales = jnp.sqrt(eigen / EXAMPLES)
    basis = jax.random.normal(jax.random.fold_in(key, 101), (count, PARAMS), jnp.float32)
    common = jax.random.normal(jax.random.fold_in(key, 103), (PARAMS,), jnp.float32)
    return (scales, basis, common)


def spread_values(key, dims):
    return jax.random.normal(key, dims, jnp.float32)


def draw_ex_grads(key, part):
    scales, basis, common = latent_setup(key)
    count = scales.shape[0]
    coeff = spread_values(jax.random.fold_in(key, 201), (EXAMPLES, count))
    noise = spread_values(jax.random.fold_in(key, 202), (EXAMPLES, PARAMS))
    loading = jax.random.uniform(jax.random.fold_in(key, 203), (EXAMPLES, 1), jnp.float32, minval=0.5, maxval=1.5)
    common_scale = 0.7
    values = jnp.dot(coeff * scales[None, :], basis) + common_scale * loading * common[None, :] + noise
    return jnp.clip(values, -6.0, 6.0).astype(jnp.bfloat16)


def draw_tgt_grads(key, part):
    scales, basis, common = latent_setup(key)
    count = scales.shape[0]
    coeff = spread_values(jax.random.fold_in(key, 301), (TARGETS, count))
    noise = spread_values(jax.random.fold_in(key, 302), (TARGETS, PARAMS))
    values = jnp.dot(coeff * scales[None, :], basis) + noise
    return jnp.clip(values, -6.0, 6.0).astype(jnp.bfloat16)


def levels(rng, shape, pieces, low, high):
    gain = 1.0
    for dim, shards_of in pieces:
        steps = jax.random.uniform(jax.random.fold_in(jax.random.fold_in(rng, 6), dim), (shards_of,), jnp.float32, low / len(pieces), high / len(pieces))
        gain = gain * jnp.repeat(jnp.exp(steps), shape[dim] // shards_of).reshape((-1,) + (1,) * (len(shape) - 1 - dim))
    return gain


def scatter_about(own_key, shape, width, reach, split=(), kind=jnp.bfloat16):
    values = width * jax.random.normal(own_key, shape, jnp.float32)
    if split:
        values = values * levels(own_key, shape, split, -0.22, 0.18)
    return jnp.clip(values, -reach, reach).astype(kind)


def setup_inputs(seed: int = 0) -> dict:
    arg_keys = jax.random.split(jax.random.key(seed), 5)
    ex_grads = draw_ex_grads(jax.random.fold_in(arg_keys[4], 71), 0)
    tgt_grads = draw_tgt_grads(jax.random.fold_in(arg_keys[4], 71), 0)
    projection = scatter_about(arg_keys[2], (PARAMS, COLS), PARAMS ** -0.5, 0.0390625, ((0, 16),))
    example_weight = jnp.clip(jnp.exp(math.log(1.0) - 2.9957323 * jax.random.uniform(arg_keys[3], (EXAMPLES,), jnp.float32) ** levels(arg_keys[3], (EXAMPLES,), ((0, 16),), -0.2, 0.2)), 0.05, 1.0)
    return dict(ex_grads=ex_grads, tgt_grads=tgt_grads, projection=projection, example_weight=example_weight)


ridge_value = 0.5

def reference(ex_grads, tgt_grads, projection, example_weight):
    train_feat = jnp.dot(ex_grads.astype(jnp.float32), projection.astype(jnp.float32), preferred_element_type=jnp.float32).astype(jnp.bfloat16)
    target_feat = jnp.dot(tgt_grads.astype(jnp.float32), projection.astype(jnp.float32), preferred_element_type=jnp.float32).astype(jnp.bfloat16)
    examples = train_feat.shape[0]
    kernel = jnp.dot(train_feat.astype(jnp.float32), train_feat.T.astype(jnp.float32), preferred_element_type=jnp.float32) / COLS
    kernel = kernel + ridge_value * jnp.eye(examples, dtype=jnp.float32)
    cross = jnp.dot(target_feat.astype(jnp.float32), train_feat.T.astype(jnp.float32), preferred_element_type=jnp.float32) / COLS
    factor = jnp.linalg.cholesky(kernel)
    forward = jax.scipy.linalg.solve_triangular(factor, cross.T, lower=True)
    solved = jax.scipy.linalg.solve_triangular(factor, forward, lower=True, trans=1)
    return solved.T * math.sqrt(COLS) * example_weight[None, :]
```

```python
import functools
import math

import jax
import jax.numpy as jnp
from jax import lax
from jax.experimental import pallas as pl
from jax.experimental.pallas import tpu as pltpu
from jax.sharding import PartitionSpec as P

ridge_value = 0.5
BLK = 128
SUB = 16


def split(x):
    hi = x.astype(jnp.bfloat16)
    return hi, (x - hi.astype(jnp.float32)).astype(jnp.bfloat16)


def dot(a, b, ca, cb):
    return lax.dot_general(a, b, (((ca,), (cb,)), ((), ())), preferred_element_type=jnp.float32)


def dot3(ah, al, bh, bl, ca, cb):
    return dot(ah, bh, ca, cb) + (dot(ah, bl, ca, cb) + dot(al, bh, ca, cb))


def factor_block(d_ref):
    rows = lax.broadcasted_iota(jnp.int32, (SUB, BLK), 0)
    for s in range(BLK // SUB):
        top = s * SUB
        left = d_ref[top : top + SUB, :BLK]
        right = d_ref[top : top + SUB, BLK:]
        cols = [jnp.broadcast_to(left[:, top + j : top + j + 1], (SUB, BLK)) for j in range(SUB)]
        for j in range(SUB):
            scale = lax.rsqrt(cols[j][j : j + 1, :])
            lower = jnp.where(rows > j, cols[j] * scale, 0.0)
            row_l = left[j : j + 1, :] * scale
            row_r = right[j : j + 1, :] * scale
            left = jnp.where(rows == j, row_l, left - lower * row_l)
            right = jnp.where(rows == j, row_r, right - lower * row_r)
            for k in range(j + 1, SUB):
                cols[k] = cols[k] - lower * lower[k : k + 1, :]
        both = jnp.concatenate([left, right], axis=1)
        d_ref[top : top + SUB, :] = both
        if s + 1 < BLK // SUB:
            hi, lo = split(both)
            lhs = jnp.concatenate([hi[:, :BLK], lo[:, :BLK], hi[:, :BLK]], axis=0)
            rhs = jnp.concatenate([hi, hi, lo], axis=0)
            update = dot(lhs, rhs, 0, 0)
            d_ref[top + SUB :, :] = d_ref[top + SUB :, :] - update[top + SUB :, :]


def chol_kernel(n, t, inverse, k_ref, y_ref, x_ref, uh, ul, row, diag, ih, il, xh, xl):
    blocks = n // BLK
    width = n + t
    ident = (
        lax.broadcasted_iota(jnp.int32, (BLK, BLK), 0) == lax.broadcasted_iota(jnp.int32, (BLK, BLK), 1)
    ).astype(jnp.float32)

    def step(k, carry):
        for kk in range(blocks):
            first = kk * BLK

            @pl.when(k == kk)
            def _(kk=kk, first=first):
                if kk == 0:
                    row[:, :n] = k_ref[:BLK, :] * inverse
                    row[:, n:] = y_ref[:BLK, :] * inverse
                else:
                    upd = dot3(
                        uh[:first, first : first + BLK],
                        ul[:first, first : first + BLK],
                        uh[:first, first:],
                        ul[:first, first:],
                        0,
                        0,
                    )
                    row[:, first:n] = k_ref[first : first + BLK, first:] * inverse - upd[:, : n - first]
                    row[:, n:] = y_ref[first : first + BLK, :] * inverse - upd[:, n - first :]
                diag[:, :BLK] = row[:, first : first + BLK] + ridge_value * ident

        diag[:, BLK:] = ident
        factor_block(diag)
        inv_h, inv_l = split(diag[:, BLK:])
        at = pl.ds(pl.multiple_of(k * BLK, BLK), BLK)
        ih[at, :] = inv_h
        il[at, :] = inv_l
        for kk in range(blocks):
            last = (kk + 1) * BLK

            @pl.when(k == kk)
            def _(kk=kk, last=last):
                a_h, a_l = split(row[:, last:])
                u = dot3(inv_h, inv_l, a_h, a_l, 1, 0)
                u_h, u_l = split(u)
                uh[last - BLK : last, last:] = u_h
                ul[last - BLK : last, last:] = u_l
                d_h, d_l = split(diag[:, :BLK])
                uh[last - BLK : last, last - BLK : last] = d_h
                ul[last - BLK : last, last - BLK : last] = d_l

        return carry

    lax.fori_loop(0, blocks, step, 0)
    for kk in reversed(range(blocks)):
        first, last = kk * BLK, (kk + 1) * BLK
        rhs = uh[first:last, n:].astype(jnp.float32) + ul[first:last, n:].astype(jnp.float32)
        if kk < blocks - 1:
            rhs = rhs - dot3(uh[first:last, last:n], ul[first:last, last:n], xh[last:, :], xl[last:, :], 1, 0)
        r_h, r_l = split(rhs)
        sol = dot3(ih[first:last, :], il[first:last, :], r_h, r_l, 0, 0)
        s_h, s_l = split(sol)
        xh[first:last, :] = s_h
        xl[first:last, :] = s_l
        x_ref[first:last, :] = sol


def chol_solve(kernel, cross_t, inverse):
    n, t = cross_t.shape
    return pl.pallas_call(
        functools.partial(chol_kernel, n, t, inverse),
        out_shape=jax.ShapeDtypeStruct((n, t), jnp.float32),
        in_specs=[pl.BlockSpec(memory_space=pltpu.VMEM)] * 2,
        out_specs=pl.BlockSpec(memory_space=pltpu.VMEM),
        scratch_shapes=[
            pltpu.VMEM((n, n + t), jnp.bfloat16),
            pltpu.VMEM((n, n + t), jnp.bfloat16),
            pltpu.VMEM((BLK, n + t), jnp.float32),
            pltpu.VMEM((BLK, 2 * BLK), jnp.float32),
            pltpu.VMEM((n, BLK), jnp.bfloat16),
            pltpu.VMEM((n, BLK), jnp.bfloat16),
            pltpu.VMEM((n, t), jnp.bfloat16),
            pltpu.VMEM((n, t), jnp.bfloat16),
        ],
        compiler_params=pltpu.CompilerParams(vmem_limit_bytes=60 * 2**20),
    )(kernel, cross_t)


def on_device(ex_grads, tgt_grads, projection, example_weight):
    ex_rows = ex_grads.shape[0]
    columns = projection.shape[1]
    params = lax.axis_size("param")
    param_pos = lax.axis_index("param")
    replicas = lax.axis_size("dp")
    stacked = jnp.concatenate([ex_grads, tgt_grads], axis=0)
    rows = stacked.shape[0]
    part = lax.dot_general(
        projection, stacked, (((0,), (1,)), ((), ())), preferred_element_type=jnp.float32
    ).astype(jnp.float16)
    parts = lax.all_to_all(part.reshape(params, columns // params, rows), "param", 0, 0, tiled=True)
    features = jnp.sum(parts.astype(jnp.float32), axis=0).astype(jnp.bfloat16)
    mine = features[:, :ex_rows]
    sent = jnp.broadcast_to(mine[None], (replicas, *mine.shape))
    everyone = jnp.moveaxis(lax.all_to_all(sent, "dp", 0, 0, tiled=True), 0, 1)
    everyone = everyone.reshape(mine.shape[0], replicas * ex_rows)
    contract = (((0,), (0,)), ((), ()))
    inner = lax.dot_general(mine, everyone, contract, preferred_element_type=jnp.float32)
    cross_t = lax.dot_general(
        everyone, features[:, ex_rows:], contract, preferred_element_type=jnp.float32
    )
    inner, cross_t = lax.psum((inner, cross_t), "param")
    kernel = lax.all_gather(inner, "dp", axis=0, tiled=True)
    solved = chol_solve(kernel, cross_t, 1.0 / columns)
    block = solved.shape[0] // params
    chosen = lax.dynamic_slice_in_dim(solved, param_pos * block, block, 0)
    return chosen.T * math.sqrt(columns) * example_weight[None, :]


def solution(mesh):
    placed = (P("dp", "param"), P("dp", "param"), P("param", None), P("param"))
    return jax.shard_map(
        on_device, mesh=mesh, in_specs=placed, out_specs=P("dp", "param"), check_vma=False
    )
```

```python
import functools
import math

import jax
import jax.numpy as jnp
from jax import lax
from jax.experimental import pallas as pl
from jax.experimental.pallas import tpu as pltpu
from jax.sharding import PartitionSpec as P

ridge_value = 0.5
BLK = 128
MESH_ID = pl.DeviceIdType.MESH
TILES = 5


def tile_place(t):
    pair, offset = t // 13, t % 13
    low = (offset + pair) // 12
    row = pair + low * (11 - 2 * pair)
    return row, row + offset - low * (12 - pair)


TILE_AT = {tile_place(t): t for t in range(78)}
SUB = 16


def split(x):
    hi = x.astype(jnp.bfloat16)
    return hi, (x - hi.astype(jnp.float32)).astype(jnp.bfloat16)


def dot(a, b, ca, cb):
    return lax.dot_general(a, b, (((ca,), (cb,)), ((), ())), preferred_element_type=jnp.float32)


def dot3(ah, al, bh, bl, ca, cb):
    return dot(ah, bh, ca, cb) + (dot(ah, bl, ca, cb) + dot(al, bh, ca, cb))


def factor_block(d_ref):
    rows = lax.broadcasted_iota(jnp.int32, (SUB, BLK), 0)
    for s in range(BLK // SUB):
        top = s * SUB
        left = d_ref[top : top + SUB, :BLK]
        right = d_ref[top : top + SUB, BLK:]
        cols = [jnp.broadcast_to(left[:, top + j : top + j + 1], (SUB, BLK)) for j in range(SUB)]
        for j in range(SUB):
            scale = lax.rsqrt(cols[j][j : j + 1, :])
            lower = jnp.where(rows > j, cols[j] * scale, 0.0)
            row_l = left[j : j + 1, :] * scale
            row_r = right[j : j + 1, :] * scale
            left = jnp.where(rows == j, row_l, left - lower * row_l)
            right = jnp.where(rows == j, row_r, right - lower * row_r)
            for k in range(j + 1, SUB):
                cols[k] = cols[k] - lower * lower[k : k + 1, :]
        both = jnp.concatenate([left, right], axis=1)
        d_ref[top : top + SUB, :] = both
        if s + 1 < BLK // SUB:
            hi, lo = split(both)
            lhs = jnp.concatenate([hi[:, :BLK], lo[:, :BLK], hi[:, :BLK]], axis=0)
            rhs = jnp.concatenate([hi, hi, lo], axis=0)
            update = dot(lhs, rhs, 0, 0)
            d_ref[top + SUB :, :] = d_ref[top + SUB :, :] - update[top + SUB :, :]


def chol_kernel(n, t, inverse, g_ref, c_ref, x_ref, uh, ul, row, diag, ih, il, xh, xl):
    blocks = n // BLK
    width = n + t
    ident = (
        lax.broadcasted_iota(jnp.int32, (BLK, BLK), 0) == lax.broadcasted_iota(jnp.int32, (BLK, BLK), 1)
    ).astype(jnp.float32)

    def step(k, carry):
        for kk in range(blocks):
            first = kk * BLK

            @pl.when(k == kk)
            def _(kk=kk, first=first):
                rhs = jnp.concatenate(
                    [c_ref[:, first : first + BLK], jnp.zeros((t - c_ref.shape[0], BLK), jnp.float32)], axis=0
                )
                row[:, n:] = rhs.T * inverse
                for cc in range(kk, blocks):
                    owner, i = divmod(TILE_AT[kk, cc], TILES)
                    for p in range(BLK // 8):
                        piece = g_ref[owner // 8 * 2 + p // 2 % 2, p // 4, owner % 8, p % 2, i]
                        row[8 * p : 8 * p + 8, cc * BLK : (cc + 1) * BLK] = piece * inverse
                if kk == 0:
                    pass
                else:
                    upd = dot3(
                        uh[:first, first : first + BLK],
                        ul[:first, first : first + BLK],
                        uh[:first, first:],
                        ul[:first, first:],
                        0,
                        0,
                    )
                    row[:, first:] = row[:, first:] - upd
                diag[:, :BLK] = row[:, first : first + BLK] + ridge_value * ident

        diag[:, BLK:] = ident
        factor_block(diag)
        inv_h, inv_l = split(diag[:, BLK:])
        at = pl.ds(pl.multiple_of(k * BLK, BLK), BLK)
        ih[at, :] = inv_h
        il[at, :] = inv_l
        for kk in range(blocks):
            last = (kk + 1) * BLK

            @pl.when(k == kk)
            def _(kk=kk, last=last):
                a_h, a_l = split(row[:, last:])
                u = dot3(inv_h, inv_l, a_h, a_l, 1, 0)
                u_h, u_l = split(u)
                uh[last - BLK : last, last:] = u_h
                ul[last - BLK : last, last:] = u_l
                d_h, d_l = split(diag[:, :BLK])
                uh[last - BLK : last, last - BLK : last] = d_h
                ul[last - BLK : last, last - BLK : last] = d_l

        return carry

    lax.fori_loop(0, blocks, step, 0)
    for kk in reversed(range(blocks)):
        first, last = kk * BLK, (kk + 1) * BLK
        rhs = uh[first:last, n:].astype(jnp.float32) + ul[first:last, n:].astype(jnp.float32)
        if kk < blocks - 1:
            rhs = rhs - dot3(uh[first:last, last:n], ul[first:last, last:n], xh[last:, :], xl[last:, :], 1, 0)
        r_h, r_l = split(rhs)
        sol = dot3(ih[first:last, :], il[first:last, :], r_h, r_l, 0, 0)
        s_h, s_l = split(sol)
        xh[first:last, :] = s_h
        xl[first:last, :] = s_l
        x_ref[first:last, :] = sol


def chol_solve(tiles, cross, inverse):
    n, t = cross.shape[1], BLK
    return pl.pallas_call(
        functools.partial(chol_kernel, n, t, inverse),
        out_shape=jax.ShapeDtypeStruct((n, t), jnp.float32),
        in_specs=[pl.BlockSpec(memory_space=pltpu.VMEM)] * 2,
        out_specs=pl.BlockSpec(memory_space=pltpu.VMEM),
        scratch_shapes=[
            pltpu.VMEM((n, n + t), jnp.bfloat16),
            pltpu.VMEM((n, n + t), jnp.bfloat16),
            pltpu.VMEM((BLK, n + t), jnp.float32),
            pltpu.VMEM((BLK, 2 * BLK), jnp.float32),
            pltpu.VMEM((n, BLK), jnp.bfloat16),
            pltpu.VMEM((n, BLK), jnp.bfloat16),
            pltpu.VMEM((n, t), jnp.bfloat16),
            pltpu.VMEM((n, t), jnp.bfloat16),
        ],
        compiler_params=pltpu.CompilerParams(vmem_limit_bytes=60 * 2**20),
    )(tiles, cross)


def finish(features, ex_rows, example_weight):
    params = lax.axis_size("param")
    columns = features.shape[1] * params
    tiles, cross = spread(features, ex_rows)
    solved = chol_solve(tiles, cross, 1.0 / columns)[:, : cross.shape[0]]
    block = solved.shape[0] // params
    chosen = jnp.swapaxes(solved.reshape(params, block, cross.shape[0]), 1, 2)
    chosen = lax.all_to_all(chosen, "param", 0, 0, tiled=True)
    return chosen.reshape(-1, block) * math.sqrt(columns) * example_weight[None, :]


def spread_kernel(feat_ref, g_ref, c_ref, fall, kp, kr, ks, kg, cp, cr, cs, cg, send, recv):
    d, p = lax.axis_index("dp"), lax.axis_index("param")
    x_hi, z = d // 8, d % 8
    y, x_lo, core = p // 4, (p // 2) % 2, p % 2
    x = x_hi * 2 + x_lo
    way = 1 - 2 * core
    ex = fall.shape[0] // 16

    def at(x, y, z, core):
        return ((x // 2) * 8 + z, (y * 2 + x % 2) * 2 + core)

    def turn(v, step, n):
        return (v + step + n) % n

    count = [0]
    started = []

    def push(src, dst, device):
        i = count[0]
        count[0] += 1
        copy = pltpu.make_async_remote_copy(
            src_ref=src,
            dst_ref=dst,
            send_sem=send.at[i],
            recv_sem=recv.at[i],
            device_id=device,
            device_id_type=MESH_ID,
        )
        copy.start()
        started.append(copy)
        return copy

    barrier = pltpu.get_barrier_semaphore()
    peers = [((d + s) % 16, p) for s in range(1, 16)]
    peers += [(d, (p + 2 * s) % 16) for s in range(1, 8)]
    peers += [(d, p + way), at(turn(x, 2 * x_lo - 1, 4), y, z, core)]
    for peer in peers:
        pl.semaphore_signal(barrier, inc=1, device_id=peer, device_id_type=MESH_ID)

    def ring(pos, n, block, device):
        got = []
        for step in range(1, n // 2 + 1):
            for copy in got:
                copy.wait_recv()
            got = []
            if step < n // 2:
                for sign in (1, -1):
                    ref = block(turn(pos, -sign * (step - 1), n))
                    got.append(push(ref, ref, device(turn(pos, sign, n))))
            else:
                ref = block((pos - way * (step - 1) + n) % n)
                got.append(push(ref, ref, device((pos + way + n) % n)))
            yield
        for copy in got:
            copy.wait_recv()
        yield

    def run(*rings):
        live = list(rings)
        while live:
            for one in list(live):
                if next(one, "end") == "end":
                    live.remove(one)

    def feat_rows(hi, zz):
        return fall.at[pl.ds(pl.multiple_of((hi * 8 + zz) * ex, ex), ex), :]

    mine = pl.ds(pl.multiple_of(d * ex, ex), ex)
    fall[mine, :] = feat_ref[:ex, :]
    pl.semaphore_wait(barrier, len(peers))

    other = (x_hi + 1) % 2

    def far_ring():
        ref = feat_rows(x_hi, z)
        copy = push(ref, ref, at(turn(x, 2, 4), y, z, core))
        yield
        copy.wait_recv()
        yield from ring(z, 8, lambda zz: feat_rows(other, zz), lambda zz: at(x, y, zz, core))

    run(
        far_ring(),
        ring(z, 8, lambda zz: feat_rows(x_hi, zz), lambda zz: at(x, y, zz, core)),
    )

    nt = (((1,), (1,)), ((), ()))
    for i in range(TILES):
        row, col = tile_place((d * TILES + i) % 78)
        a = fall[pl.ds(pl.multiple_of(row * 128, 128), 128), :]
        b = fall[pl.ds(pl.multiple_of(col * 128, 128), 128), :]
        tile = lax.dot_general(a, b, nt, preferred_element_type=jnp.float32)
        kp[:, :, i] = tile.reshape(8, 2, 8, 128)
    k_core = push(kp.at[:, 1 - core], kr, (d, p + way))
    cross = lax.dot_general(feat_ref[ex:, :], fall[...], nt, preferred_element_type=jnp.float32)
    cp[...] = cross.reshape(cp.shape)
    c_core = push(cp.at[:, 1 - core], cr, (d, p + way))

    chip = p // 2

    def chips(pieces, landing):
        return [
            push(pieces.at[(chip + s) % 8], landing.at[s - 1], (d, (p + 2 * s) % 16))
            for s in (4, 5, 3, 2, 6, 1, 7)
        ]

    k_core.wait_recv()
    ks[...] = kp[:, core] + kr[...]
    k_parts = chips(ks, kg)
    c_core.wait_recv()
    cs[...] = cp[:, core] + cr[...]
    for copy in k_parts:
        copy.wait_recv()
    total = ks[chip]
    for s in range(7):
        total = total + kg[s]
    g_ref[x, y, z, core] = total
    c_parts = chips(cs, cg)

    run(ring(z, 8, lambda zz: g_ref.at[x, y, zz, core], lambda zz: at(x, y, zz, core)))
    low, high = pl.ds(0, 4), pl.ds(4, 4)
    run(
        ring(x, 4, lambda xx: g_ref.at[xx, y, low, core], lambda xx: at(xx, y, z, core)),
        ring(y, 4, lambda yy: g_ref.at[x, yy, high, core], lambda yy: at(x, yy, z, core)),
    )
    pair = (d, p + way)
    shared = []

    def pass_on(ref):
        shared.append(push(ref, ref, pair))

    pass_on(g_ref.at[:, y, low, core])
    pass_on(g_ref.at[x, :, high, core])
    last_y = lambda yy: g_ref.at[:, yy, low, core]
    last_x = lambda xx: g_ref.at[xx, :, high, core]
    ring_y = ring(y, 4, last_y, lambda yy: at(x, yy, z, core))
    ring_x = ring(x, 4, last_x, lambda xx: at(xx, y, z, core))
    next(ring_y)
    next(ring_x)
    next(ring_y)
    for sign in (1, -1):
        pass_on(last_y(turn(y, sign, 4)))
    next(ring_x)
    for sign in (1, -1):
        pass_on(last_x(turn(x, sign, 4)))
    next(ring_y)
    pass_on(last_y(turn(y, 2, 4)))
    next(ring_x)
    pass_on(last_x(turn(x, 2, 4)))
    for copy in c_parts:
        copy.wait_recv()
    whole = cs[chip]
    for s in range(7):
        whole = whole + cg[s]
    c_ref[...] = whole
    for copy in shared:
        copy.wait_recv()
    for copy in started:
        copy.wait_send()


def spread(features, ex):
    width = features.shape[1]
    tgt = (features.shape[0] - ex) // 16
    n = 16 * ex
    f32 = jnp.float32
    return pl.pallas_call(
        spread_kernel,
        out_shape=(
            jax.ShapeDtypeStruct((4, 4, 8, 2, TILES, 8, 128), f32),
            jax.ShapeDtypeStruct((tgt, n), f32),
        ),
        in_specs=[pl.BlockSpec(memory_space=pltpu.VMEM)],
        out_specs=(pl.BlockSpec(memory_space=pltpu.VMEM), pl.BlockSpec(memory_space=pltpu.VMEM)),
        scratch_shapes=[
            pltpu.VMEM((n, width), jnp.bfloat16),
            pltpu.VMEM((8, 2, TILES, 8, 128), f32),
            pltpu.VMEM((8, TILES, 8, 128), f32),
            pltpu.VMEM((8, TILES, 8, 128), f32),
            pltpu.VMEM((7, TILES, 8, 128), f32),
            pltpu.VMEM((8, 2, tgt, n), f32),
            pltpu.VMEM((8, tgt, n), f32),
            pltpu.VMEM((8, tgt, n), f32),
            pltpu.VMEM((7, tgt, n), f32),
            pltpu.SemaphoreType.DMA((60,)),
            pltpu.SemaphoreType.DMA((60,)),
        ],
        compiler_params=pltpu.CompilerParams(
            collective_id=0, has_side_effects=True, vmem_limit_bytes=60 * 2**20
        ),
    )(features)


def on_device(ex_grads, tgt_grads, projection, example_weight):
    ex_rows = ex_grads.shape[0]
    columns = projection.shape[1]
    params = lax.axis_size("param")
    stacked = jnp.concatenate([ex_grads, tgt_grads], axis=0)
    rows = stacked.shape[0]
    part = jnp.dot(stacked, projection, preferred_element_type=jnp.float32).astype(jnp.float16)
    part = jnp.moveaxis(part.reshape(rows, params, columns // params), 1, 0)
    parts = lax.all_to_all(part, "param", 0, 0, tiled=True)
    features = jnp.sum(parts.astype(jnp.float32), axis=0).astype(jnp.bfloat16)
    return finish(features, ex_rows, example_weight)


def solution(mesh):
    placed = (P("dp", "param"), P("dp", "param"), P("param", None), P("param"))
    return jax.shard_map(
        on_device, mesh=mesh, in_specs=placed, out_specs=P("dp", "param"), check_vma=False
    )
```

```python
import functools
import math

import jax
import jax.numpy as jnp
from jax import lax
from jax.experimental import pallas as pl
from jax.experimental.pallas import tpu as pltpu
from jax.sharding import PartitionSpec as P

ridge_value = 0.5
BLK = 128
SUB = 16
TILES = 5
LATE_SUM = 8
F32, BF16 = jnp.float32, jnp.bfloat16


def tile_place(t):
    pair, offset = t // 13, t % 13
    low = (offset + pair) // 12
    row = pair + low * (11 - 2 * pair)
    return row, row + offset - low * (12 - pair)


TILE_AT = {tile_place(t): t for t in range(78)}


def split(x):
    hi = x.astype(BF16)
    return hi, (x - hi.astype(F32)).astype(BF16)


def dot(a, b, ca, cb):
    return lax.dot_general(a, b, (((ca,), (cb,)), ((), ())), preferred_element_type=F32)


def dot3(ah, al, bh, bl, ca, cb):
    return dot(ah, bh, ca, cb) + (dot(ah, bl, ca, cb) + dot(al, bh, ca, cb))


def factor_block(d_ref):
    rows = lax.broadcasted_iota(jnp.int32, (SUB, BLK), 0)
    for s in range(BLK // SUB):
        top = s * SUB
        left = d_ref[top : top + SUB, :BLK]
        right = d_ref[top : top + SUB, BLK:]
        cols = [jnp.broadcast_to(left[:, top + j : top + j + 1], (SUB, BLK)) for j in range(SUB)]
        for j in range(SUB):
            scale = lax.rsqrt(cols[j][j : j + 1, :])
            lower = jnp.where(rows > j, cols[j] * scale, 0.0)
            row_l = left[j : j + 1, :] * scale
            row_r = right[j : j + 1, :] * scale
            left = jnp.where(rows == j, row_l, left - lower * row_l)
            right = jnp.where(rows == j, row_r, right - lower * row_r)
            for k in range(j + 1, SUB):
                cols[k] = cols[k] - lower * lower[k : k + 1, :]
        both = jnp.concatenate([left, right], axis=1)
        d_ref[top : top + SUB, :] = both
        if s + 1 < BLK // SUB:
            hi, lo = split(both)
            lhs = jnp.concatenate([hi[:, :BLK], lo[:, :BLK], hi[:, :BLK]], axis=0)
            rhs = jnp.concatenate([hi, hi, lo], axis=0)
            update = dot(lhs, rhs, 0, 0)
            d_ref[top + SUB :, :] = d_ref[top + SUB :, :] - update[top + SUB :, :]


def scores_kernel(
    inverse, out_scale, ex_ref, tgt_ref, proj_ref, w_ref, o_ref,
    stack, pv, ep, er, eg, tp, tr, tg, fall, tfeat, kp, kr, kg, g, cp, cr, cg,
    uh, ul, row, diag, ih, il, yh, yl, xh, xl, xo, og, load, send, recv,
):
    d, p = lax.axis_index("dp"), lax.axis_index("param")
    x_hi, z = d // 8, d % 8
    y, x_lo, core = p // 4, (p // 2) % 2, p % 2
    x = x_hi * 2 + x_lo
    way = 1 - 2 * core
    chip = p // 2
    pair = (d, p + way)
    n, width = fall.shape
    ex = n // 16
    blocks = n // BLK

    def at(x, y, z, core):
        return ((x // 2) * 8 + z, (y * 2 + x % 2) * 2 + core)

    def turn(v, step, n):
        return (v + step + n) % n

    started = []

    def push(src, dst, device, now=True):
        i = len(started)
        copy = pltpu.make_async_remote_copy(
            src_ref=src,
            dst_ref=dst,
            send_sem=send.at[i],
            recv_sem=recv.at[i],
            device_id=device,
            device_id_type=pl.DeviceIdType.MESH,
        )
        if now:
            copy.start()
        started.append(copy)
        return copy

    def landed(copies):
        for copy in copies:
            copy.wait_recv()

    def ring(pos, n, block, device):
        got = []
        for step in range(1, n // 2 + 1):
            landed(got)
            got = []
            if step < n // 2:
                for sign in (1, -1):
                    ref = block(turn(pos, -sign * (step - 1), n))
                    got.append(push(ref, ref, device(turn(pos, sign, n))))
            else:
                ref = block((pos - way * (step - 1) + n) % n)
                got.append(push(ref, ref, device((pos + way + n) % n)))
            yield
        landed(got)
        yield

    def run(*rings):
        live = list(rings)
        while live:
            for one in list(live):
                if next(one, "end") == "end":
                    live.remove(one)

    def chips(pieces, landing, steps=(4, 5, 3, 2, 6, 1, 7), now=True):
        return [
            push(pieces.at[(chip + s) % 8], landing.at[s - 1], (d, (p + 2 * s) % 16), now) for s in steps
        ]

    def summed(pieces, landing):
        total = pieces[chip]
        for s in range(7):
            total = total + landing[s]
        return total

    barrier = pltpu.get_barrier_semaphore()
    peers = [((d + s) % 16, p) for s in range(1, 16)]
    peers += [(d, (p + s) % 16) for s in range(1, 16)]
    peers += [at(turn(x, 2 * x_lo - 1, 4), y, z, core)]
    for peer in peers:
        pl.semaphore_signal(barrier, inc=1, device_id=peer, device_id_type=pl.DeviceIdType.MESH)

    loads = [
        pltpu.make_async_copy(ex_ref, stack.at[:ex], load.at[16]),
        pltpu.make_async_copy(tgt_ref, stack.at[ex:], load.at[17]),
    ]
    for j in range(16):
        owner = 2 * (j % 8) + (1 - core if j < 8 else core)
        span = pl.ds(pl.multiple_of(owner * width, width), width)
        loads.append(pltpu.make_async_copy(proj_ref.at[:, span], pv.at[j], load.at[j]))
    for copy in loads:
        copy.start()
    loads[0].wait()
    loads[1].wait()
    pl.semaphore_wait(barrier, len(peers))

    e_pair = []
    for j in range(16):
        loads[2 + j].wait()
        part = dot(stack[...], pv[j], 1, 0)
        side = 0 if j < 8 else 1
        ep[side, j % 8] = part[:ex]
        tp[side, j % 8] = part[ex:]
        if j < 8:
            e_pair.append(push(ep.at[0, j], er.at[j], pair))
    t_pair = push(tp.at[0], tr, pair)
    landed(e_pair)
    er[...] = er[...] + ep[1]
    e_parts = chips(er, eg)
    landed([t_pair])
    tr[...] = tr[...] + tp[1]
    landed(e_parts)
    mine = pl.ds(pl.multiple_of(d * ex, ex), ex)
    fall[mine, :] = summed(er, eg).astype(BF16)
    t_parts = chips(tr, tg, (4, 2, 6))

    def feat_rows(hi, zz):
        return fall.at[pl.ds(pl.multiple_of((hi * 8 + zz) * ex, ex), ex), :]

    other = (x_hi + 1) % 2

    def far_ring():
        ref = feat_rows(x_hi, z)
        copy = push(ref, ref, at(turn(x, 2, 4), y, z, core))
        yield
        copy.wait_recv()
        yield from ring(z, 8, lambda zz: feat_rows(other, zz), lambda zz: at(x, y, zz, core))

    run(
        far_ring(),
        ring(z, 8, lambda zz: feat_rows(x_hi, zz), lambda zz: at(x, y, zz, core)),
    )

    for i in range(TILES):
        r, c = tile_place((d * TILES + i) % 78)
        a = fall[pl.ds(pl.multiple_of(r * BLK, BLK), BLK), :]
        b = fall[pl.ds(pl.multiple_of(c * BLK, BLK), BLK), :]
        kp[:, :, i] = dot(a, b, 1, 1).reshape(8, 2, 8, BLK)
    k_pair = push(kp.at[:, 1 - core], kr, pair)
    landed([k_pair])
    kr[...] = kr[...] + kp[:, core]
    landed(chips(kr, kg))
    g[x, y, z, core] = summed(kr, kg)

    run(ring(z, 8, lambda zz: g.at[x, y, zz, core], lambda zz: at(x, y, zz, core)))
    low, high = pl.ds(0, 4), pl.ds(4, 4)
    run(
        ring(x, 4, lambda xx: g.at[xx, y, low, core], lambda xx: at(xx, y, z, core)),
        ring(y, 4, lambda yy: g.at[x, yy, high, core], lambda yy: at(x, yy, z, core)),
    )
    shared = []

    def pass_on(ref):
        shared.append(push(ref, ref, pair))

    def last_y(yy):
        return g.at[:, yy, low, core]

    def last_x(xx):
        return g.at[xx, :, high, core]

    pass_on(last_y(y))
    pass_on(last_x(x))
    ring_y = ring(y, 4, last_y, lambda yy: at(x, yy, z, core))
    ring_x = ring(x, 4, last_x, lambda xx: at(xx, y, z, core))
    next(ring_y)
    next(ring_x)
    next(ring_y)
    for sign in (1, -1):
        pass_on(last_y(turn(y, sign, 4)))
    next(ring_x)
    for sign in (1, -1):
        pass_on(last_x(turn(x, sign, 4)))
    next(ring_y)
    pass_on(last_y(turn(y, 2, 4)))
    next(ring_x)
    pass_on(last_x(turn(x, 2, 4)))
    landed(shared)
    t_parts += chips(tr, tg, (5, 3, 1, 7))

    ident = (
        lax.broadcasted_iota(jnp.int32, (BLK, BLK), 0) == lax.broadcasted_iota(jnp.int32, (BLK, BLK), 1)
    ).astype(F32)
    c_pair = push(cp.at[:, 1 - core], cr, pair, False)
    c_parts = chips(cr, cg, now=False)

    def step(k, carry):
        @pl.when(k == LATE_SUM)
        def _():
            landed(t_parts)
            tfeat[...] = summed(tr, tg).astype(BF16)
            cp[...] = dot(tfeat[...], fall[...], 1, 1).reshape(cp.shape)
            c_pair.start()

        @pl.when(k == LATE_SUM + 1)
        def _():
            landed([c_pair])
            cr[...] = cr[...] + cp[:, core]
            for copy in c_parts:
                copy.start()

        for kk in range(blocks):
            first = kk * BLK

            @pl.when(k == kk)
            def _(kk=kk, first=first):
                for cc in range(kk, blocks):
                    owner, i = divmod(TILE_AT[kk, cc], TILES)
                    for q in range(BLK // 8):
                        piece = g[owner // 8 * 2 + q // 2 % 2, q // 4, owner % 8, q % 2, i]
                        row[8 * q : 8 * q + 8, cc * BLK : (cc + 1) * BLK] = piece * inverse
                if kk:
                    upd = dot3(
                        uh[:first, first : first + BLK],
                        ul[:first, first : first + BLK],
                        uh[:first, first:],
                        ul[:first, first:],
                        0,
                        0,
                    )
                    row[:, first:] = row[:, first:] - upd
                diag[:, :BLK] = row[:, first : first + BLK] + ridge_value * ident

        diag[:, BLK:] = ident
        factor_block(diag)
        inv_h, inv_l = split(diag[:, BLK:])
        place = pl.ds(pl.multiple_of(k * BLK, BLK), BLK)
        ih[place, :] = inv_h
        il[place, :] = inv_l
        for kk in range(blocks - 1):
            last = (kk + 1) * BLK

            @pl.when(k == kk)
            def _(last=last):
                a_h, a_l = split(row[:, last:])
                u_h, u_l = split(dot3(inv_h, inv_l, a_h, a_l, 1, 0))
                uh[last - BLK : last, last:] = u_h
                ul[last - BLK : last, last:] = u_l

        return carry

    lax.fori_loop(0, blocks, step, 0)

    landed(c_parts)
    cross = summed(cr, cg) * inverse

    def against(vh, vl, mh, ml, cm):
        both = dot(jnp.concatenate([vh, vl], axis=0), mh, 1, cm)
        half = vh.shape[0]
        return both[:half] + (both[half:] + dot(vh, ml, 1, cm))

    for kk in range(blocks):
        first, last = kk * BLK, (kk + 1) * BLK
        v = cross[:, first:last]
        if kk:
            v = v - against(yh[:, :first], yl[:, :first], uh[:first, first:last], ul[:first, first:last], 0)
        v_h, v_l = split(v)
        v = against(v_h, v_l, ih[first:last, :], il[first:last, :], 1)
        v_h, v_l = split(v)
        yh[:, first:last] = v_h
        yl[:, first:last] = v_l
    for kk in reversed(range(blocks)):
        first, last = kk * BLK, (kk + 1) * BLK
        v = yh[:, first:last].astype(F32) + yl[:, first:last].astype(F32)
        if kk < blocks - 1:
            v = v - against(xh[:, last:], xl[:, last:], uh[first:last, last:], ul[first:last, last:], 1)
        v_h, v_l = split(v)
        v = against(v_h, v_l, ih[first:last, :], il[first:last, :], 0)
        v_h, v_l = split(v)
        xh[:, first:last] = v_h
        xl[:, first:last] = v_l
        row[:16, first:last] = v

    for q in range(16):
        xo[q, :, :ex] = row[:16, q * ex : (q + 1) * ex]
    finals = [push(xo.at[(p + s) % 16], og.at[s - 1], (d, (p + s) % 16)) for s in range(1, 16)]
    weight = w_ref[...] * out_scale
    o_ref[pl.ds(pl.multiple_of(p * 16, 16), 16), :] = xo[p][:, :ex] * weight
    for s in range(1, 16):
        finals[s - 1].wait_recv()
        o_ref[pl.ds(pl.multiple_of((p + 16 - s) % 16 * 16, 16), 16), :] = og[s - 1][:, :ex] * weight
    for copy in started:
        copy.wait_send()


def on_device(ex_grads, tgt_grads, projection, example_weight):
    ex, depth = ex_grads.shape
    tgt = tgt_grads.shape[0]
    columns = projection.shape[1]
    n, width, rhs = 16 * ex, columns // 16, tgt // 16
    vmem, anywhere = pl.BlockSpec(memory_space=pltpu.VMEM), pl.BlockSpec(memory_space=pl.ANY)
    scratch = [
        ((ex + tgt, depth), BF16),
        ((16, depth, width), BF16),
        ((2, 8, ex, width), F32),
        ((8, ex, width), F32),
        ((7, ex, width), F32),
        ((2, 8, tgt, width), F32),
        ((8, tgt, width), F32),
        ((7, tgt, width), F32),
        ((n, width), BF16),
        ((tgt, width), BF16),
        ((8, 2, TILES, 8, BLK), F32),
        ((8, TILES, 8, BLK), F32),
        ((7, TILES, 8, BLK), F32),
        ((4, 4, 8, 2, TILES, 8, BLK), F32),
        ((8, 2, rhs, n), F32),
        ((8, rhs, n), F32),
        ((7, rhs, n), F32),
        ((n, n), BF16),
        ((n, n), BF16),
        ((BLK, n), F32),
        ((BLK, 2 * BLK), F32),
        ((n, BLK), BF16),
        ((n, BLK), BF16),
        ((rhs, n), BF16),
        ((rhs, n), BF16),
        ((rhs, n), BF16),
        ((rhs, n), BF16),
        ((16, rhs, BLK), F32),
        ((15, rhs, BLK), F32),
    ]
    return pl.pallas_call(
        functools.partial(scores_kernel, 1.0 / columns, math.sqrt(columns)),
        out_shape=jax.ShapeDtypeStruct((tgt, ex), F32),
        in_specs=[anywhere, anywhere, anywhere, vmem],
        out_specs=vmem,
        scratch_shapes=[pltpu.VMEM(*one) for one in scratch]
        + [
            pltpu.SemaphoreType.DMA((18,)),
            pltpu.SemaphoreType.DMA((96,)),
            pltpu.SemaphoreType.DMA((96,)),
        ],
        compiler_params=pltpu.CompilerParams(
            collective_id=0, has_side_effects=True, vmem_limit_bytes=63 * 2**20
        ),
    )(ex_grads, tgt_grads, projection, example_weight.reshape(1, ex))


def solution(mesh):
    placed = (P("dp", "param"), P("dp", "param"), P("param", None), P("param"))
    return jax.shard_map(
        on_device, mesh=mesh, in_specs=placed, out_specs=P("dp", "param"), check_vma=False
    )
```

```python
import functools
import math

import jax
import jax.numpy as jnp
from jax import lax
from jax.experimental import pallas as pl
from jax.experimental.pallas import tpu as pltpu
from jax.sharding import PartitionSpec as P

ridge_value = 0.5
BLK = 128
SUB = 16
TILES = 5
LATE_SUM = 8
F32, BF16 = jnp.float32, jnp.bfloat16


def tile_place(t):
    pair, offset = t // 13, t % 13
    low = (offset + pair) // 12
    row = pair + low * (11 - 2 * pair)
    return row, row + offset - low * (12 - pair)


TILE_AT = {tile_place(t): t for t in range(78)}


def split(x):
    hi = x.astype(BF16)
    return hi, (x - hi.astype(F32)).astype(BF16)


def dot(a, b, ca, cb):
    return lax.dot_general(a, b, (((ca,), (cb,)), ((), ())), preferred_element_type=F32)


def dot3(ah, al, bh, bl, ca, cb):
    return dot(ah, bh, ca, cb) + (dot(ah, bl, ca, cb) + dot(al, bh, ca, cb))


def factor_block(d_ref):
    rows = lax.broadcasted_iota(jnp.int32, (SUB, BLK), 0)
    for s in range(BLK // SUB):
        top = s * SUB
        left = d_ref[top : top + SUB, :BLK]
        right = d_ref[top : top + SUB, BLK:]
        cols = [jnp.broadcast_to(left[:, top + j : top + j + 1], (SUB, BLK)) for j in range(SUB)]
        for j in range(SUB):
            scale = lax.rsqrt(cols[j][j : j + 1, :])
            lower = jnp.where(rows > j, cols[j] * scale, 0.0)
            row_l = left[j : j + 1, :] * scale
            row_r = right[j : j + 1, :] * scale
            left = jnp.where(rows == j, row_l, left - lower * row_l)
            right = jnp.where(rows == j, row_r, right - lower * row_r)
            for k in range(j + 1, SUB):
                cols[k] = cols[k] - lower * lower[k : k + 1, :]
        both = jnp.concatenate([left, right], axis=1)
        d_ref[top : top + SUB, :] = both
        if s + 1 < BLK // SUB:
            hi, lo = split(both)
            lhs = jnp.concatenate([hi[:, :BLK], lo[:, :BLK], hi[:, :BLK]], axis=0)
            rhs = jnp.concatenate([hi, hi, lo], axis=0)
            update = dot(lhs, rhs, 0, 0)
            d_ref[top + SUB :, :] = d_ref[top + SUB :, :] - update[top + SUB :, :]


def scores_kernel(
    inverse, out_scale, ex_ref, tgt_ref, proj_ref, w_ref, o_ref,
    stack, pv, ep, er, eg, tp, tr, tg, fall, tfeat, kp, kr, kg, g, cp, cr, cg,
    uh, ul, row, diag, ih, il, yh, yl, xh, xl, xo, og, load, send, recv,
):
    d, p = lax.axis_index("dp"), lax.axis_index("param")
    x_hi, z = d // 8, d % 8
    y, x_lo, core = p // 4, (p // 2) % 2, p % 2
    x = x_hi * 2 + x_lo
    way = 1 - 2 * core
    chip = p // 2
    pair = (d, p + way)
    n, width = fall.shape
    ex = n // 16
    blocks = n // BLK

    def at(x, y, z, core):
        return ((x // 2) * 8 + z, (y * 2 + x % 2) * 2 + core)

    def turn(v, step, n):
        return (v + step + n) % n

    started = []

    def push(src, dst, device, now=True):
        i = len(started)
        copy = pltpu.make_async_remote_copy(
            src_ref=src,
            dst_ref=dst,
            send_sem=send.at[i],
            recv_sem=recv.at[i],
            device_id=device,
            device_id_type=pl.DeviceIdType.MESH,
        )
        if now:
            copy.start()
        started.append(copy)
        return copy

    def landed(copies):
        for copy in copies:
            copy.wait_recv()

    def ring(pos, n, block, device):
        got = []
        for step in range(1, n // 2 + 1):
            landed(got)
            got = []
            if step < n // 2:
                for sign in (1, -1):
                    ref = block(turn(pos, -sign * (step - 1), n))
                    got.append(push(ref, ref, device(turn(pos, sign, n))))
            else:
                ref = block((pos - way * (step - 1) + n) % n)
                got.append(push(ref, ref, device((pos + way + n) % n)))
            yield
        landed(got)
        yield

    def run(*rings):
        live = list(rings)
        while live:
            for one in list(live):
                if next(one, "end") == "end":
                    live.remove(one)

    def chips(pieces, landing, steps=(4, 5, 3, 2, 6, 1, 7), now=True):
        return [
            push(pieces.at[(chip + s) % 8], landing.at[s - 1], (d, (p + 2 * s) % 16), now) for s in steps
        ]

    def summed(pieces, landing):
        total = pieces[chip]
        for s in range(7):
            total = total + landing[s]
        return total

    barrier = pltpu.get_barrier_semaphore()
    peers = [at(x, y, (z + s) % 8, core) for s in range(1, 8)]
    peers += [(d, (p + s) % 16) for s in range(1, 16)]
    peers += [at(turn(x, 2 * x_lo - 1, 4), y, z, core), at(turn(x, 2, 4), y, z, core)]
    for peer in peers:
        pl.semaphore_signal(barrier, inc=1, device_id=peer, device_id_type=pl.DeviceIdType.MESH)

    loads = [
        pltpu.make_async_copy(ex_ref, stack.at[:ex], load.at[8]),
        pltpu.make_async_copy(tgt_ref, stack.at[ex:], load.at[9]),
    ]
    for j in range(8):
        span = pl.ds(2 * j * width, 2 * width)
        loads.append(pltpu.make_async_copy(proj_ref.at[:, span], pv.at[j], load.at[j]))
    for copy in loads:
        copy.start()
    loads[0].wait()
    loads[1].wait()
    for j in range(8):
        loads[2 + j].wait()
        part = dot(stack[...], pv[j], 1, 0)
        for c in range(2):
            ep[c, j] = part[:ex, c * width : (c + 1) * width]
            tp[c, j] = part[ex:, c * width : (c + 1) * width]
    pl.semaphore_wait(barrier, len(peers))

    e_pair = push(ep.at[1 - core], er, pair)
    t_pair = push(tp.at[1 - core], tr, pair)
    landed([e_pair])
    er[...] = er[...] + ep[core]
    e_parts = chips(er, eg)
    landed([t_pair])
    tr[...] = tr[...] + tp[core]
    landed(e_parts)
    mine = pl.ds(pl.multiple_of(d * ex, ex), ex)
    fall[mine, :] = summed(er, eg).astype(BF16)
    t_parts = chips(tr, tg, (4, 2, 6))

    def feat_rows(hi, zz):
        return fall.at[pl.ds(pl.multiple_of((hi * 8 + zz) * ex, ex), ex), :]

    other = (x_hi + 1) % 2

    def far_ring():
        ref = feat_rows(x_hi, z)
        copy = push(ref, ref, at(turn(x, 2, 4), y, z, core))
        yield
        copy.wait_recv()
        yield from ring(z, 8, lambda zz: feat_rows(other, zz), lambda zz: at(x, y, zz, core))

    run(
        far_ring(),
        ring(z, 8, lambda zz: feat_rows(x_hi, zz), lambda zz: at(x, y, zz, core)),
    )

    for i in range(TILES):
        r, c = tile_place((d * TILES + i) % 78)
        a = fall[pl.ds(pl.multiple_of(r * BLK, BLK), BLK), :]
        b = fall[pl.ds(pl.multiple_of(c * BLK, BLK), BLK), :]
        kp[:, :, i] = dot(a, b, 1, 1).reshape(8, 2, 8, BLK)
    k_pair = push(kp.at[:, 1 - core], kr, pair)
    landed([k_pair])
    kr[...] = kr[...] + kp[:, core]
    landed(chips(kr, kg))
    g[x, y, z, core] = summed(kr, kg)

    own = g.at[x, y, z, core]
    landed([push(own, own, at(x, y, (z + s) % 8, core)) for s in (4, 3, 5, 2, 6, 1, 7)])
    low, high = pl.ds(0, 4), pl.ds(4, 4)
    run(
        ring(x, 4, lambda xx: g.at[xx, y, low, core], lambda xx: at(xx, y, z, core)),
        ring(y, 4, lambda yy: g.at[x, yy, high, core], lambda yy: at(x, yy, z, core)),
    )
    shared = []

    def pass_on(ref):
        shared.append(push(ref, ref, pair))

    def last_y(yy):
        return g.at[:, yy, low, core]

    def last_x(xx):
        return g.at[xx, :, high, core]

    pass_on(last_y(y))
    pass_on(last_x(x))
    ring_y = ring(y, 4, last_y, lambda yy: at(x, yy, z, core))
    ring_x = ring(x, 4, last_x, lambda xx: at(xx, y, z, core))
    next(ring_y)
    next(ring_x)
    next(ring_y)
    for sign in (1, -1):
        pass_on(last_y(turn(y, sign, 4)))
    next(ring_x)
    for sign in (1, -1):
        pass_on(last_x(turn(x, sign, 4)))
    next(ring_y)
    pass_on(last_y(turn(y, 2, 4)))
    next(ring_x)
    pass_on(last_x(turn(x, 2, 4)))
    landed(shared)
    t_parts += chips(tr, tg, (5, 3, 1, 7))

    ident = (
        lax.broadcasted_iota(jnp.int32, (BLK, BLK), 0) == lax.broadcasted_iota(jnp.int32, (BLK, BLK), 1)
    ).astype(F32)
    c_pair = push(cp.at[:, 1 - core], cr, pair, False)
    c_parts = chips(cr, cg, now=False)

    def step(k, carry):
        @pl.when(k == LATE_SUM)
        def _():
            landed(t_parts)
            tfeat[...] = summed(tr, tg).astype(BF16)
            cp[...] = dot(tfeat[...], fall[...], 1, 1).reshape(cp.shape)
            c_pair.start()

        @pl.when(k == LATE_SUM + 1)
        def _():
            landed([c_pair])
            cr[...] = cr[...] + cp[:, core]
            for copy in c_parts:
                copy.start()

        for kk in range(blocks):
            first = kk * BLK

            @pl.when(k == kk)
            def _(kk=kk, first=first):
                for cc in range(kk, blocks):
                    owner, i = divmod(TILE_AT[kk, cc], TILES)
                    for q in range(BLK // 8):
                        piece = g[owner // 8 * 2 + q // 2 % 2, q // 4, owner % 8, q % 2, i]
                        row[8 * q : 8 * q + 8, cc * BLK : (cc + 1) * BLK] = piece * inverse
                if kk:
                    upd = dot3(
                        uh[:first, first : first + BLK],
                        ul[:first, first : first + BLK],
                        uh[:first, first:],
                        ul[:first, first:],
                        0,
                        0,
                    )
                    row[:, first:] = row[:, first:] - upd
                diag[:, :BLK] = row[:, first : first + BLK] + ridge_value * ident

        diag[:, BLK:] = ident
        factor_block(diag)
        inv_h, inv_l = split(diag[:, BLK:])
        place = pl.ds(pl.multiple_of(k * BLK, BLK), BLK)
        ih[place, :] = inv_h
        il[place, :] = inv_l
        for kk in range(blocks - 1):
            last = (kk + 1) * BLK

            @pl.when(k == kk)
            def _(last=last):
                a_h, a_l = split(row[:, last:])
                u_h, u_l = split(dot3(inv_h, inv_l, a_h, a_l, 1, 0))
                uh[last - BLK : last, last:] = u_h
                ul[last - BLK : last, last:] = u_l

        return carry

    lax.fori_loop(0, blocks, step, 0)

    landed(c_parts)
    cross = summed(cr, cg) * inverse

    def against(vh, vl, mh, ml, cm):
        both = dot(jnp.concatenate([vh, vl], axis=0), mh, 1, cm)
        half = vh.shape[0]
        return both[:half] + (both[half:] + dot(vh, ml, 1, cm))

    for kk in range(blocks):
        first, last = kk * BLK, (kk + 1) * BLK
        v = cross[:, first:last]
        if kk:
            v = v - against(yh[:, :first], yl[:, :first], uh[:first, first:last], ul[:first, first:last], 0)
        v_h, v_l = split(v)
        v = against(v_h, v_l, ih[first:last, :], il[first:last, :], 1)
        v_h, v_l = split(v)
        yh[:, first:last] = v_h
        yl[:, first:last] = v_l
    for kk in reversed(range(blocks)):
        first, last = kk * BLK, (kk + 1) * BLK
        v = yh[:, first:last].astype(F32) + yl[:, first:last].astype(F32)
        if kk < blocks - 1:
            v = v - against(xh[:, last:], xl[:, last:], uh[first:last, last:], ul[first:last, last:], 1)
        v_h, v_l = split(v)
        v = against(v_h, v_l, ih[first:last, :], il[first:last, :], 0)
        v_h, v_l = split(v)
        xh[:, first:last] = v_h
        xl[:, first:last] = v_l
        row[:16, first:last] = v

    for q in range(16):
        xo[q, :, :ex] = row[:16, q * ex : (q + 1) * ex]
    finals = [push(xo.at[(p + s) % 16], og.at[s - 1], (d, (p + s) % 16)) for s in range(1, 16)]
    weight = w_ref[...] * out_scale
    o_ref[pl.ds(pl.multiple_of(p * 16, 16), 16), :] = xo[p][:, :ex] * weight
    for s in range(1, 16):
        finals[s - 1].wait_recv()
        o_ref[pl.ds(pl.multiple_of((p + 16 - s) % 16 * 16, 16), 16), :] = og[s - 1][:, :ex] * weight
    for copy in started:
        copy.wait_send()


def on_device(ex_grads, tgt_grads, projection, example_weight):
    ex, depth = ex_grads.shape
    tgt = tgt_grads.shape[0]
    columns = projection.shape[1]
    n, width, rhs = 16 * ex, columns // 16, tgt // 16
    vmem, anywhere = pl.BlockSpec(memory_space=pltpu.VMEM), pl.BlockSpec(memory_space=pl.ANY)
    scratch = [
        ((ex + tgt, depth), BF16),
        ((8, depth, 2 * width), BF16),
        ((2, 8, ex, width), F32),
        ((8, ex, width), F32),
        ((7, ex, width), F32),
        ((2, 8, tgt, width), F32),
        ((8, tgt, width), F32),
        ((7, tgt, width), F32),
        ((n, width), BF16),
        ((tgt, width), BF16),
        ((8, 2, TILES, 8, BLK), F32),
        ((8, TILES, 8, BLK), F32),
        ((7, TILES, 8, BLK), F32),
        ((4, 4, 8, 2, TILES, 8, BLK), F32),
        ((8, 2, rhs, n), F32),
        ((8, rhs, n), F32),
        ((7, rhs, n), F32),
        ((n, n), BF16),
        ((n, n), BF16),
        ((BLK, n), F32),
        ((BLK, 2 * BLK), F32),
        ((n, BLK), BF16),
        ((n, BLK), BF16),
        ((rhs, n), BF16),
        ((rhs, n), BF16),
        ((rhs, n), BF16),
        ((rhs, n), BF16),
        ((16, rhs, BLK), F32),
        ((15, rhs, BLK), F32),
    ]
    return pl.pallas_call(
        functools.partial(scores_kernel, 1.0 / columns, math.sqrt(columns)),
        out_shape=jax.ShapeDtypeStruct((tgt, ex), F32),
        in_specs=[anywhere, anywhere, anywhere, vmem],
        out_specs=vmem,
        scratch_shapes=[pltpu.VMEM(*one) for one in scratch]
        + [
            pltpu.SemaphoreType.DMA((10,)),
            pltpu.SemaphoreType.DMA((96,)),
            pltpu.SemaphoreType.DMA((96,)),
        ],
        compiler_params=pltpu.CompilerParams(
            collective_id=0, has_side_effects=True, vmem_limit_bytes=63 * 2**20
        ),
    )(ex_grads, tgt_grads, projection, example_weight.reshape(1, ex))


def solution(mesh):
    placed = (P("dp", "param"), P("dp", "param"), P("param", None), P("param"))
    return jax.shard_map(
        on_device, mesh=mesh, in_specs=placed, out_specs=P("dp", "param"), check_vma=False
    )
```

```python
import functools
import math

import jax
import jax.numpy as jnp
from jax import lax
from jax.experimental import pallas as pl
from jax.experimental.pallas import tpu as pltpu
from jax.sharding import PartitionSpec as P

ridge_value = 0.5
BLK = 128
SUB = 16
TILES = 5
LATE_SUM = 8
F32, BF16 = jnp.float32, jnp.bfloat16


def tile_place(t):
    row, first = 0, 0
    for q in range(1, 12):
        past = (t + 80 - (12 * q - q * (q - 1) // 2)) // 80
        row = row + past
        first = first + past * (13 - q)
    return row, row + t - first


def tile_owner(t):
    rank, slot = divmod(t, TILES)
    half, rest = divmod(rank, 8)
    return rest // 4, half * 4 + rest % 4, slot


TILE_AT = {tile_place(t): t for t in range(78)}


def split(x):
    hi = x.astype(BF16)
    return hi, (x - hi.astype(F32)).astype(BF16)


def dot(a, b, ca, cb):
    return lax.dot_general(a, b, (((ca,), (cb,)), ((), ())), preferred_element_type=F32)


def dot3(ah, al, bh, bl, ca, cb):
    return dot(ah, bh, ca, cb) + (dot(ah, bl, ca, cb) + dot(al, bh, ca, cb))


def factor_block(d_ref):
    rows = lax.broadcasted_iota(jnp.int32, (SUB, BLK), 0)
    subs = BLK // SUB
    own = d_ref[:SUB, :]
    for s in range(subs):
        top = s * SUB
        left, right = own[:, :BLK], own[:, BLK:]
        cols = [jnp.broadcast_to(left[:, top + j : top + j + 1], (SUB, BLK)) for j in range(SUB)]
        lowers, scales, row_ls, row_rs = [], [], [], []
        for j in range(SUB):
            scale = lax.rsqrt(cols[j][j : j + 1, :])
            lower = jnp.where(rows > j, cols[j] * scale, 0.0)
            row_l = left[j : j + 1, :] * scale
            row_r = right[j : j + 1, :] * scale
            left = jnp.where(rows == j, row_l, left - lower * row_l)
            right = jnp.where(rows == j, row_r, right - lower * row_r)
            for k in range(j + 1, SUB):
                cols[k] = cols[k] - lower * lower[k : k + 1, :]
            lowers.append(lower)
            scales.append(scale)
            row_ls.append(row_l)
            row_rs.append(row_r)
        if s + 1 < subs:
            nxt = d_ref[top + SUB : top + 2 * SUB, :]
            next_l, next_r = nxt[:, :BLK], nxt[:, BLK:]
            below = [jnp.broadcast_to(next_l[:, top + j : top + j + 1], (SUB, BLK)) for j in range(SUB)]
            for j in range(SUB):
                lower = below[j] * scales[j]
                next_l = next_l - lower * row_ls[j]
                next_r = next_r - lower * row_rs[j]
                for k in range(j + 1, SUB):
                    below[k] = below[k] - lower * lowers[j][k : k + 1, :]
            own = jnp.concatenate([next_l, next_r], axis=1)
        both = jnp.concatenate([left, right], axis=1)
        d_ref[top : top + SUB, :] = both
        if s + 2 < subs:
            hi, lo = split(both)
            lhs = jnp.concatenate([hi[:, :BLK], lo[:, :BLK], hi[:, :BLK]], axis=0)
            rhs = jnp.concatenate([hi, hi, lo], axis=0)
            update = dot(lhs, rhs, 0, 0)
            d_ref[top + 2 * SUB :, :] = d_ref[top + 2 * SUB :, :] - update[top + 2 * SUB :, :]


def scores_kernel(
    inverse, out_scale, ex_ref, tgt_ref, proj_ref, w_ref, o_ref,
    stack, pv, ep, er, eg, tp, tr, tg, fall, tfeat, kp, kr, kg, g, cp, cr, cg,
    uh, ul, row, diag, ih, il, yh, yl, xh, xl, xo, og, load, send, recv,
):
    d, p = lax.axis_index("dp"), lax.axis_index("param")
    x_hi, z = d // 8, d % 8
    y, x_lo, core = p // 4, (p // 2) % 2, p % 2
    x = x_hi * 2 + x_lo
    way = 1 - 2 * core
    chip = p // 2
    pair = (d, p + way)
    n, width = fall.shape
    ex = n // 16
    blocks = n // BLK

    def at(x, y, z, core):
        return ((x // 2) * 8 + z, (y * 2 + x % 2) * 2 + core)

    def turn(v, step, n):
        return (v + step + n) % n

    started = []
    later = [None]

    def act(copy, name):
        if later[0] is None:
            getattr(copy, name)()
        else:
            later[0].append((copy, name))

    def recorded(gen):
        parts = []
        for live in [True] * 16:
            later[0] = []
            live = next(gen, "end") != "end"
            parts.append(later[0])
            if not live:
                break
        later[0] = None
        return parts

    def replay(part):
        for copy, name in part:
            getattr(copy, name)()

    def push(src, dst, device, now=True):
        i = len(started)
        copy = pltpu.make_async_remote_copy(
            src_ref=src,
            dst_ref=dst,
            send_sem=send.at[i],
            recv_sem=recv.at[i],
            device_id=device,
            device_id_type=pl.DeviceIdType.MESH,
        )
        if now:
            act(copy, "start")
        started.append(copy)
        return copy

    def landed(copies):
        for copy in copies:
            act(copy, "wait_recv")

    def ring(pos, n, block, device):
        got = []
        for step in range(1, n // 2 + 1):
            landed(got)
            got = []
            if step < n // 2:
                for sign in (1, -1):
                    ref = block(turn(pos, -sign * (step - 1), n))
                    got.append(push(ref, ref, device(turn(pos, sign, n))))
            else:
                ref = block((pos - way * (step - 1) + n) % n)
                got.append(push(ref, ref, device((pos + way + n) % n)))
            yield
        landed(got)
        yield

    def run(*rings):
        live = list(rings)
        while live:
            for one in list(live):
                if next(one, "end") == "end":
                    live.remove(one)

    def chips(pieces, landing, steps=(4, 5, 3, 2, 6, 1, 7), now=True):
        return [
            push(pieces.at[(chip + s) % 8], landing.at[s - 1], (d, (p + 2 * s) % 16), now) for s in steps
        ]

    def summed(pieces, landing):
        total = pieces[chip]
        for s in range(7):
            total = total + landing[s]
        return total

    barrier = pltpu.get_barrier_semaphore()
    peers = [at(x, y, (z + s) % 8, core) for s in range(1, 8)]
    peers += [(d, (p + s) % 16) for s in range(1, 16)]
    peers += [at(turn(x, 2 * x_lo - 1, 4), y, z, core), at(turn(x, 2, 4), y, z, core)]
    for peer in peers:
        pl.semaphore_signal(barrier, inc=1, device_id=peer, device_id_type=pl.DeviceIdType.MESH)

    loads = [
        pltpu.make_async_copy(ex_ref, stack.at[:ex], load.at[8]),
        pltpu.make_async_copy(tgt_ref, stack.at[ex:], load.at[9]),
    ]
    for j in range(8):
        span = pl.ds(2 * j * width, 2 * width)
        loads.append(pltpu.make_async_copy(proj_ref.at[:, span], pv.at[j], load.at[j]))
    for copy in loads:
        copy.start()
    loads[0].wait()
    loads[1].wait()
    for j in range(8):
        loads[2 + j].wait()
        part = dot(stack[...], pv[j], 1, 0)
        for c in range(2):
            ep[c, j] = part[:ex, c * width : (c + 1) * width]
            tp[c, j] = part[ex:, c * width : (c + 1) * width]
    pl.semaphore_wait(barrier, len(peers))

    e_pair = push(ep.at[1 - core], er, pair)
    landed([e_pair])
    er[...] = er[...] + ep[core]
    e_parts = chips(er, eg)
    t_pair = push(tp.at[1 - core], tr, pair)
    landed([t_pair])
    tr[...] = tr[...] + tp[core]
    landed(e_parts)
    mine = pl.ds(pl.multiple_of(d * ex, ex), ex)
    fall[mine, :] = summed(er, eg).astype(BF16)
    t_parts = chips(tr, tg, (3, 5, 7))

    def feat_rows(hi, zz):
        return fall.at[pl.ds(pl.multiple_of((hi * 8 + zz) * ex, ex), ex), :]

    other = (x_hi + 1) % 2

    def far_ring():
        ref = feat_rows(x_hi, z)
        copy = push(ref, ref, at(turn(x, 2, 4), y, z, core))
        yield
        copy.wait_recv()
        yield from ring(z, 8, lambda zz: feat_rows(other, zz), lambda zz: at(x, y, zz, core))

    run(
        far_ring(),
        ring(z, 8, lambda zz: feat_rows(x_hi, zz), lambda zz: at(x, y, zz, core)),
    )

    for i in range(TILES):
        r, c = tile_place(((z // 4 * 8 + x_hi * 4 + z % 4) * TILES + i) % 78)
        a = fall[pl.ds(pl.multiple_of(r * BLK, BLK), BLK), :]
        b = fall[pl.ds(pl.multiple_of(c * BLK, BLK), BLK), :]
        kp[:, :, i] = dot(a, b, 1, 1).reshape(8, 2, 8, BLK)
    k_pair = push(kp.at[:, 1 - core], kr, pair)
    landed([k_pair])
    kr[...] = kr[...] + kp[:, core]
    landed(chips(kr, kg))
    g[x, y, z, core] = summed(kr, kg)

    own = g.at[x, y, z, core]
    landed([push(own, own, at(x, y, (z + s) % 8, core)) for s in (4, 3, 5, 2, 6, 1, 7)])

    def gather(base):
        one, two = pl.ds(base, 2), pl.ds(base + 2, 2)

        def to_x(xx):
            return at(xx, y, z, core)

        def to_y(yy):
            return at(x, yy, z, core)

        def last_y(yy):
            return g.at[:, yy, one, core]

        def last_x(xx):
            return g.at[xx, :, two, core]

        shared = []

        def pass_on(ref):
            shared.append(push(ref, ref, pair))

        first_x = ring(x, 4, lambda xx: g.at[xx, y, one, core], to_x)
        first_y = ring(y, 4, lambda yy: g.at[x, yy, two, core], to_y)
        next(first_x)
        next(first_y)
        yield
        next(first_x)
        next(first_y)
        yield
        next(first_x)
        next(first_y)
        ring_y, ring_x = ring(y, 4, last_y, to_y), ring(x, 4, last_x, to_x)
        next(ring_y)
        next(ring_x)
        pass_on(last_y(y))
        pass_on(last_x(x))
        yield
        next(ring_y)
        next(ring_x)
        for sign in (1, -1):
            pass_on(last_y(turn(y, sign, 4)))
            pass_on(last_x(turn(x, sign, 4)))
        yield
        next(ring_y)
        pass_on(last_y(turn(y, 2, 4)))
        next(ring_x)
        pass_on(last_x(turn(x, 2, 4)))
        landed(shared)
        yield

    for _ in gather(0):
        pass
    rest = recorded(gather(4))
    replay(rest[0])
    t_rest = chips(tr, tg, (4, 1, 2, 6), now=False)
    t_parts += t_rest

    ident = (
        lax.broadcasted_iota(jnp.int32, (BLK, BLK), 0) == lax.broadcasted_iota(jnp.int32, (BLK, BLK), 1)
    ).astype(F32)
    c_pair = push(cp.at[:, 1 - core], cr, pair, False)
    c_parts = chips(cr, cg, now=False)

    def step(k, carry):
        @pl.when(k == 1)
        def _():
            replay(rest[2])

        @pl.when(k == 3)
        def _():
            replay(rest[4])
            replay(rest[5])
            for copy in t_rest:
                copy.start()

        @pl.when(k == LATE_SUM)
        def _():
            landed(t_parts)
            tfeat[...] = summed(tr, tg).astype(BF16)
            cp[...] = dot(tfeat[...], fall[...], 1, 1).reshape(cp.shape)
            c_pair.start()

        @pl.when(k == LATE_SUM + 1)
        def _():
            landed([c_pair])
            cr[...] = cr[...] + cp[:, core]
            for copy in c_parts:
                copy.start()

        for kk in range(blocks):
            first = kk * BLK

            @pl.when(k == kk)
            def _(kk=kk, first=first):
                for cc in range(kk, blocks):
                    o_hi, o_z, i = tile_owner(TILE_AT[kk, cc])
                    for q in range(BLK // 8):
                        piece = g[o_hi * 2 + q // 2 % 2, q // 4, o_z, q % 2, i]
                        row[8 * q : 8 * q + 8, cc * BLK : (cc + 1) * BLK] = piece * inverse
                if kk:
                    upd = dot3(
                        uh[:first, first : first + BLK],
                        ul[:first, first : first + BLK],
                        uh[:first, first:],
                        ul[:first, first:],
                        0,
                        0,
                    )
                    row[:, first:] = row[:, first:] - upd
                diag[:, :BLK] = row[:, first : first + BLK] + ridge_value * ident

        diag[:, BLK:] = ident
        factor_block(diag)

        @pl.when(k == 0)
        def _():
            replay(rest[1])

        @pl.when(k == 2)
        def _():
            replay(rest[3])

        inv_h, inv_l = split(diag[:, BLK:])
        place = pl.ds(pl.multiple_of(k * BLK, BLK), BLK)
        ih[place, :] = inv_h
        il[place, :] = inv_l
        for kk in range(blocks - 1):
            last = (kk + 1) * BLK

            @pl.when(k == kk)
            def _(last=last):
                a_h, a_l = split(row[:, last:])
                u_h, u_l = split(dot3(inv_h, inv_l, a_h, a_l, 1, 0))
                uh[last - BLK : last, last:] = u_h
                ul[last - BLK : last, last:] = u_l

        return carry

    lax.fori_loop(0, blocks, step, 0)

    landed(c_parts)
    cross = summed(cr, cg) * inverse

    def against(vh, vl, mh, ml, cm):
        both = dot(jnp.concatenate([vh, vl], axis=0), mh, 1, cm)
        half = vh.shape[0]
        return both[:half] + (both[half:] + dot(vh, ml, 1, cm))

    for kk in range(blocks):
        first, last = kk * BLK, (kk + 1) * BLK
        v = cross[:, first:last]
        if kk:
            v = v - against(yh[:, :first], yl[:, :first], uh[:first, first:last], ul[:first, first:last], 0)
        v_h, v_l = split(v)
        v = against(v_h, v_l, ih[first:last, :], il[first:last, :], 1)
        v_h, v_l = split(v)
        yh[:, first:last] = v_h
        yl[:, first:last] = v_l
    for kk in reversed(range(blocks)):
        first, last = kk * BLK, (kk + 1) * BLK
        v = yh[:, first:last].astype(F32) + yl[:, first:last].astype(F32)
        if kk < blocks - 1:
            v = v - against(xh[:, last:], xl[:, last:], uh[first:last, last:], ul[first:last, last:], 1)
        v_h, v_l = split(v)
        v = against(v_h, v_l, ih[first:last, :], il[first:last, :], 0)
        v_h, v_l = split(v)
        xh[:, first:last] = v_h
        xl[:, first:last] = v_l
        row[:16, first:last] = v

    for q in range(16):
        xo[q, :, :ex] = row[:16, q * ex : (q + 1) * ex]
    finals = [push(xo.at[(p + s) % 16], og.at[s - 1], (d, (p + s) % 16)) for s in range(1, 16)]
    weight = w_ref[...] * out_scale
    o_ref[pl.ds(pl.multiple_of(p * 16, 16), 16), :] = xo[p][:, :ex] * weight
    for s in range(1, 16):
        finals[s - 1].wait_recv()
        o_ref[pl.ds(pl.multiple_of((p + 16 - s) % 16 * 16, 16), 16), :] = og[s - 1][:, :ex] * weight
    for copy in started:
        copy.wait_send()


def on_device(ex_grads, tgt_grads, projection, example_weight):
    ex, depth = ex_grads.shape
    tgt = tgt_grads.shape[0]
    columns = projection.shape[1]
    n, width, rhs = 16 * ex, columns // 16, tgt // 16
    vmem, anywhere = pl.BlockSpec(memory_space=pltpu.VMEM), pl.BlockSpec(memory_space=pl.ANY)
    scratch = [
        ((ex + tgt, depth), BF16),
        ((8, depth, 2 * width), BF16),
        ((2, 8, ex, width), F32),
        ((8, ex, width), F32),
        ((7, ex, width), F32),
        ((2, 8, tgt, width), F32),
        ((8, tgt, width), F32),
        ((7, tgt, width), F32),
        ((n, width), BF16),
        ((tgt, width), BF16),
        ((8, 2, TILES, 8, BLK), F32),
        ((8, TILES, 8, BLK), F32),
        ((7, TILES, 8, BLK), F32),
        ((4, 4, 8, 2, TILES, 8, BLK), F32),
        ((8, 2, rhs, n), F32),
        ((8, rhs, n), F32),
        ((7, rhs, n), F32),
        ((n, n), BF16),
        ((n, n), BF16),
        ((BLK, n), F32),
        ((BLK, 2 * BLK), F32),
        ((n, BLK), BF16),
        ((n, BLK), BF16),
        ((rhs, n), BF16),
        ((rhs, n), BF16),
        ((rhs, n), BF16),
        ((rhs, n), BF16),
        ((16, rhs, BLK), F32),
        ((15, rhs, BLK), F32),
    ]
    return pl.pallas_call(
        functools.partial(scores_kernel, 1.0 / columns, math.sqrt(columns)),
        out_shape=jax.ShapeDtypeStruct((tgt, ex), F32),
        in_specs=[anywhere, anywhere, anywhere, vmem],
        out_specs=vmem,
        scratch_shapes=[pltpu.VMEM(*one) for one in scratch]
        + [
            pltpu.SemaphoreType.DMA((10,)),
            pltpu.SemaphoreType.DMA((112,)),
            pltpu.SemaphoreType.DMA((112,)),
        ],
        compiler_params=pltpu.CompilerParams(
            collective_id=0, has_side_effects=True, vmem_limit_bytes=63 * 2**20
        ),
    )(ex_grads, tgt_grads, projection, example_weight.reshape(1, ex))


def solution(mesh):
    placed = (P("dp", "param"), P("dp", "param"), P("param", None), P("param"))
    return jax.shard_map(
        on_device, mesh=mesh, in_specs=placed, out_specs=P("dp", "param"), check_vma=False
    )
```

```python
import functools
import math

import jax
import jax.numpy as jnp
from jax import lax
from jax.experimental import pallas as pl
from jax.experimental.pallas import tpu as pltpu
from jax.sharding import PartitionSpec as P

ridge_value = 0.5
BLK = 128
SUB = 16
TILES = 5
LATE_SUM = 8
F32, BF16 = jnp.float32, jnp.bfloat16


def tile_place(t):
    row, first = 0, 0
    for q in range(1, 12):
        past = (t + 80 - (12 * q - q * (q - 1) // 2)) // 80
        row = row + past
        first = first + past * (13 - q)
    return row, row + t - first


def tile_owner(t):
    rank, slot = divmod(t, TILES)
    half, rest = divmod(rank, 8)
    return rest // 4, half * 4 + rest % 4, slot


TILE_AT = {tile_place(t): t for t in range(78)}


def split(x):
    hi = x.astype(BF16)
    return hi, (x - hi.astype(F32)).astype(BF16)


def dot(a, b, ca, cb):
    return lax.dot_general(a, b, (((ca,), (cb,)), ((), ())), preferred_element_type=F32)


def dot3(ah, al, bh, bl, ca, cb):
    return dot(ah, bh, ca, cb) + (dot(ah, bl, ca, cb) + dot(al, bh, ca, cb))


def factor_block(d_ref):
    rows = lax.broadcasted_iota(jnp.int32, (SUB, BLK), 0)
    subs = BLK // SUB
    own = d_ref[:SUB, :]
    for s in range(subs):
        top = s * SUB
        left, right = own[:, :BLK], own[:, BLK:]
        cols = [jnp.broadcast_to(left[:, top + j : top + j + 1], (SUB, BLK)) for j in range(SUB)]
        lowers, scales, row_ls, row_rs = [], [], [], []
        for j in range(SUB):
            scale = lax.rsqrt(cols[j][j : j + 1, :])
            lower = jnp.where(rows > j, cols[j] * scale, 0.0)
            row_l = left[j : j + 1, :] * scale
            row_r = right[j : j + 1, :] * scale
            left = jnp.where(rows == j, row_l, left - lower * row_l)
            right = jnp.where(rows == j, row_r, right - lower * row_r)
            for k in range(j + 1, SUB):
                cols[k] = cols[k] - lower * lower[k : k + 1, :]
            lowers.append(lower)
            scales.append(scale)
            row_ls.append(row_l)
            row_rs.append(row_r)
        if s + 1 < subs:
            nxt = d_ref[top + SUB : top + 2 * SUB, :]
            next_l, next_r = nxt[:, :BLK], nxt[:, BLK:]
            below = [jnp.broadcast_to(next_l[:, top + j : top + j + 1], (SUB, BLK)) for j in range(SUB)]
            for j in range(SUB):
                lower = below[j] * scales[j]
                next_l = next_l - lower * row_ls[j]
                next_r = next_r - lower * row_rs[j]
                for k in range(j + 1, SUB):
                    below[k] = below[k] - lower * lowers[j][k : k + 1, :]
            own = jnp.concatenate([next_l, next_r], axis=1)
        both = jnp.concatenate([left, right], axis=1)
        d_ref[top : top + SUB, :] = both
        if s + 2 < subs:
            hi, lo = split(both)
            lhs = jnp.concatenate([hi[:, :BLK], lo[:, :BLK], hi[:, :BLK]], axis=0)
            rhs = jnp.concatenate([hi, hi, lo], axis=0)
            update = dot(lhs, rhs, 0, 0)
            d_ref[top + 2 * SUB :, :] = d_ref[top + 2 * SUB :, :] - update[top + 2 * SUB :, :]


def scores_kernel(
    inverse, out_scale, ex_ref, tgt_ref, proj_ref, w_ref, o_ref,
    stack, pv, ep, er, eg, tp, tr, tg, fall, tfeat, kp, kr, kg, g, cp, cr, cg,
    uh, ul, row, diag, ih, il, yh, yl, xh, xl, xo, og, load, send, recv,
):
    d, p = lax.axis_index("dp"), lax.axis_index("param")
    x_hi, z = d // 8, d % 8
    y, x_lo, core = p // 4, (p // 2) % 2, p % 2
    x = x_hi * 2 + x_lo
    way = 1 - 2 * core
    chip = p // 2
    pair = (d, p + way)
    n, width = fall.shape
    ex = n // 16
    blocks = n // BLK

    def at(x, y, z, core):
        return ((x // 2) * 8 + z, (y * 2 + x % 2) * 2 + core)

    def turn(v, step, n):
        return (v + step + n) % n

    started = []
    later = [None]

    def act(copy, name):
        if later[0] is None:
            getattr(copy, name)()
        else:
            later[0].append((copy, name))

    def recorded(gen):
        parts = []
        for live in [True] * 16:
            later[0] = []
            live = next(gen, "end") != "end"
            parts.append(later[0])
            if not live:
                break
        later[0] = None
        return parts

    def replay(part):
        for copy, name in part:
            getattr(copy, name)()

    def push(src, dst, device, now=True):
        i = len(started)
        copy = pltpu.make_async_remote_copy(
            src_ref=src,
            dst_ref=dst,
            send_sem=send.at[i],
            recv_sem=recv.at[i],
            device_id=device,
            device_id_type=pl.DeviceIdType.MESH,
        )
        if now:
            act(copy, "start")
        started.append(copy)
        return copy

    def landed(copies):
        for copy in copies:
            act(copy, "wait_recv")

    def run(*rings):
        live = list(rings)
        while live:
            for one in list(live):
                if next(one, "end") == "end":
                    live.remove(one)

    def chips(pieces, landing, steps=(4, 5, 3, 2, 6, 1, 7), now=True):
        return [
            push(pieces.at[(chip + s) % 8], landing.at[s - 1], (d, (p + 2 * s) % 16), now) for s in steps
        ]

    def summed(pieces, landing):
        total = pieces[chip]
        for s in range(7):
            total = total + landing[s]
        return total

    barrier = pltpu.get_barrier_semaphore()
    peers = [at(x, y, (z + s) % 8, core) for s in range(1, 8)]
    peers += [(d, (p + s) % 16) for s in range(1, 16)]
    peers += [at(turn(x, 2 * x_lo - 1, 4), y, z, core), at(turn(x, 2, 4), y, z, core)]
    for peer in peers:
        pl.semaphore_signal(barrier, inc=1, device_id=peer, device_id_type=pl.DeviceIdType.MESH)

    loads = [
        pltpu.make_async_copy(ex_ref, stack.at[:ex], load.at[8]),
        pltpu.make_async_copy(tgt_ref, stack.at[ex:], load.at[9]),
    ]
    for j in range(8):
        span = pl.ds(2 * j * width, 2 * width)
        loads.append(pltpu.make_async_copy(proj_ref.at[:, span], pv.at[j], load.at[j]))
    for copy in loads:
        copy.start()
    loads[0].wait()
    loads[1].wait()
    for j in range(8):
        loads[2 + j].wait()
        part = dot(stack[...], pv[j], 1, 0)
        for c in range(2):
            ep[c, j] = part[:ex, c * width : (c + 1) * width]
            tp[c, j] = part[ex:, c * width : (c + 1) * width]
    pl.semaphore_wait(barrier, len(peers))

    e_pair = push(ep.at[1 - core], er, pair)
    landed([e_pair])
    er[...] = er[...] + ep[core]
    e_parts = chips(er, eg)
    t_pair = push(tp.at[1 - core], tr, pair)
    landed([t_pair])
    tr[...] = tr[...] + tp[core]
    landed(e_parts)
    mine = pl.ds(pl.multiple_of(d * ex, ex), ex)
    fall[mine, :] = summed(er, eg).astype(BF16)

    def feat_rows(hi, zz):
        return fall.at[pl.ds(pl.multiple_of((hi * 8 + zz) * ex, ex), ex), :]

    other = (x_hi + 1) % 2

    ref = feat_rows(x_hi, z)
    far = push(ref, ref, at(turn(x, 2, 4), y, z, core))
    t_parts = chips(tr, tg, (3, 5))

    def along_z(hi):
        own = feat_rows(hi, z)
        near = [push(own, own, at(x, y, turn(z, step, 8), core)) for step in (2, -2, 1, -1)]
        yield
        landed(near)
        back = [feat_rows(hi, turn(z, -2, 8)), feat_rows(hi, turn(z, 2, 8))]
        away = feat_rows(hi, (z - 2 * way + 8) % 8)
        near = [
            push(away, away, at(x, y, (z + 2 * way + 8) % 8, core)),
            push(back[0], back[0], at(x, y, turn(z, 1, 8), core)),
            push(back[1], back[1], at(x, y, turn(z, -1, 8), core)),
        ]
        yield
        landed(near)
        yield

    def far_z():
        far.wait_recv()
        yield from along_z(other)

    run(along_z(x_hi), far_z())

    for i in range(TILES):
        r, c = tile_place(((z // 4 * 8 + x_hi * 4 + z % 4) * TILES + i) % 78)
        a = fall[pl.ds(pl.multiple_of(r * BLK, BLK), BLK), :]
        b = fall[pl.ds(pl.multiple_of(c * BLK, BLK), BLK), :]
        kp[:, :, i] = dot(a, b, 1, 1).reshape(8, 2, 8, BLK)
    k_pair = push(kp.at[:, 1 - core], kr, pair)
    landed([k_pair])
    kr[...] = kr[...] + kp[:, core]
    landed(chips(kr, kg))
    g[x, y, z, core] = summed(kr, kg)

    own = g.at[x, y, z, core]
    landed([push(own, own, at(x, y, (z + s) % 8, core)) for s in (4, 3, 5, 2, 6, 1, 7)])

    def gather(base):
        one, two = pl.ds(base, 2), pl.ds(base + 2, 2)

        def to_x(xx):
            return at(xx, y, z, core)

        def to_y(yy):
            return at(x, yy, z, core)

        def last_y(yy):
            return g.at[:, yy, one, core]

        def last_x(xx):
            return g.at[xx, :, two, core]

        shared = []

        def pass_on(ref):
            shared.append(push(ref, ref, pair))

        def to_all(pos, block, device):
            ref = block(pos)
            return [push(ref, ref, device((pos + step) % 4)) for step in (2, 1, 3)]

        first = to_all(x, lambda xx: g.at[xx, y, one, core], to_x)
        first += to_all(y, lambda yy: g.at[x, yy, two, core], to_y)
        yield
        landed(first)
        by_y, by_x = to_all(y, last_y, to_y), to_all(x, last_x, to_x)
        pass_on(last_y(y))
        pass_on(last_x(x))
        yield
        for i, step in ((1, 3), (2, 1), (0, 2)):
            landed([by_y[i]])
            pass_on(last_y((y + step) % 4))
            landed([by_x[i]])
            pass_on(last_x((x + step) % 4))
        landed(shared)
        yield

    for _ in gather(0):
        pass
    rest = recorded(gather(4))
    replay(rest[0])
    t_rest = chips(tr, tg, (4, 1, 7, 2, 6), now=False)
    t_parts += t_rest

    ident = (
        lax.broadcasted_iota(jnp.int32, (BLK, BLK), 0) == lax.broadcasted_iota(jnp.int32, (BLK, BLK), 1)
    ).astype(F32)

    def late_tile(r, c):
        return r == 3 and TILE_AT[r, c] >= 8 * TILES

    def tile_rows(r, c, q):
        o_hi, o_z, i = tile_owner(TILE_AT[r, c])
        return g[o_hi * 2 + q // 2 % 2, q // 4, o_z, q % 2, i] * inverse

    c_pair = push(cp.at[:, 1 - core], cr, pair, False)
    c_parts = chips(cr, cg, now=False)

    def step(k, carry):
        @pl.when(k == 1)
        def _():
            replay(rest[1])

        @pl.when(k == LATE_SUM)
        def _():
            landed(t_parts)
            tfeat[...] = summed(tr, tg).astype(BF16)
            cp[...] = dot(tfeat[...], fall[...], 1, 1).reshape(cp.shape)
            c_pair.start()

        @pl.when(k == LATE_SUM + 1)
        def _():
            landed([c_pair])
            cr[...] = cr[...] + cp[:, core]
            for copy in c_parts:
                copy.start()

        for kk in range(blocks):
            first = kk * BLK

            @pl.when(k == kk)
            def _(kk=kk, first=first):
                for cc in range(kk, blocks):
                    span = slice(cc * BLK, (cc + 1) * BLK)
                    if late_tile(kk, cc):
                        row[:, span] = jnp.zeros((BLK, BLK), F32)
                        continue
                    for q in range(BLK // 8):
                        row[8 * q : 8 * q + 8, span] = tile_rows(kk, cc, q)
                if kk:
                    upd = dot3(
                        uh[:first, first : first + BLK],
                        ul[:first, first : first + BLK],
                        uh[:first, first:],
                        ul[:first, first:],
                        0,
                        0,
                    )
                    row[:, first:] = row[:, first:] - upd
                diag[:, :BLK] = row[:, first : first + BLK] + ridge_value * ident

        diag[:, BLK:] = ident
        factor_block(diag)

        @pl.when(k == 3)
        def _():
            replay(rest[2])
            for copy in t_rest:
                copy.start()

        inv_h, inv_l = split(diag[:, BLK:])
        place = pl.ds(pl.multiple_of(k * BLK, BLK), BLK)
        ih[place, :] = inv_h
        il[place, :] = inv_l
        for kk in range(blocks - 1):
            last = (kk + 1) * BLK

            @pl.when(k == kk)
            def _(kk=kk, last=last):
                for cc in range(kk, blocks):
                    span = slice(cc * BLK, (cc + 1) * BLK)
                    if late_tile(kk, cc):
                        for q in range(BLK // 8):
                            row[8 * q : 8 * q + 8, span] += tile_rows(kk, cc, q)
                a_h, a_l = split(row[:, last:])
                u_h, u_l = split(dot3(inv_h, inv_l, a_h, a_l, 1, 0))
                uh[last - BLK : last, last:] = u_h
                ul[last - BLK : last, last:] = u_l

        return carry

    lax.fori_loop(0, blocks, step, 0)

    landed(c_parts)
    cross = summed(cr, cg) * inverse

    def against(vh, vl, mh, ml, cm):
        both = dot(jnp.concatenate([vh, vl], axis=0), mh, 1, cm)
        half = vh.shape[0]
        return both[:half] + (both[half:] + dot(vh, ml, 1, cm))

    for kk in range(blocks):
        first, last = kk * BLK, (kk + 1) * BLK
        v = cross[:, first:last]
        if kk:
            v = v - against(yh[:, :first], yl[:, :first], uh[:first, first:last], ul[:first, first:last], 0)
        v_h, v_l = split(v)
        v = against(v_h, v_l, ih[first:last, :], il[first:last, :], 1)
        v_h, v_l = split(v)
        yh[:, first:last] = v_h
        yl[:, first:last] = v_l
    for kk in reversed(range(blocks)):
        first, last = kk * BLK, (kk + 1) * BLK
        v = yh[:, first:last].astype(F32) + yl[:, first:last].astype(F32)
        if kk < blocks - 1:
            v = v - against(xh[:, last:], xl[:, last:], uh[first:last, last:], ul[first:last, last:], 1)
        v_h, v_l = split(v)
        v = against(v_h, v_l, ih[first:last, :], il[first:last, :], 0)
        v_h, v_l = split(v)
        xh[:, first:last] = v_h
        xl[:, first:last] = v_l
        row[:16, first:last] = v

    for q in range(16):
        xo[q, :, :ex] = row[:16, q * ex : (q + 1) * ex]
    finals = [push(xo.at[(p + s) % 16], og.at[s - 1], (d, (p + s) % 16)) for s in range(1, 16)]
    weight = w_ref[...] * out_scale
    o_ref[pl.ds(pl.multiple_of(p * 16, 16), 16), :] = xo[p][:, :ex] * weight
    for s in range(1, 16):
        finals[s - 1].wait_recv()
        o_ref[pl.ds(pl.multiple_of((p + 16 - s) % 16 * 16, 16), 16), :] = og[s - 1][:, :ex] * weight
    for copy in started:
        copy.wait_send()


def on_device(ex_grads, tgt_grads, projection, example_weight):
    ex, depth = ex_grads.shape
    tgt = tgt_grads.shape[0]
    columns = projection.shape[1]
    n, width, rhs = 16 * ex, columns // 16, tgt // 16
    vmem, anywhere = pl.BlockSpec(memory_space=pltpu.VMEM), pl.BlockSpec(memory_space=pl.ANY)
    scratch = [
        ((ex + tgt, depth), BF16),
        ((8, depth, 2 * width), BF16),
        ((2, 8, ex, width), F32),
        ((8, ex, width), F32),
        ((7, ex, width), F32),
        ((2, 8, tgt, width), F32),
        ((8, tgt, width), F32),
        ((7, tgt, width), F32),
        ((n, width), BF16),
        ((tgt, width), BF16),
        ((8, 2, TILES, 8, BLK), F32),
        ((8, TILES, 8, BLK), F32),
        ((7, TILES, 8, BLK), F32),
        ((4, 4, 8, 2, TILES, 8, BLK), F32),
        ((8, 2, rhs, n), F32),
        ((8, rhs, n), F32),
        ((7, rhs, n), F32),
        ((n, n), BF16),
        ((n, n), BF16),
        ((BLK, n), F32),
        ((BLK, 2 * BLK), F32),
        ((n, BLK), BF16),
        ((n, BLK), BF16),
        ((rhs, n), BF16),
        ((rhs, n), BF16),
        ((rhs, n), BF16),
        ((rhs, n), BF16),
        ((16, rhs, BLK), F32),
        ((15, rhs, BLK), F32),
    ]
    return pl.pallas_call(
        functools.partial(scores_kernel, 1.0 / columns, math.sqrt(columns)),
        out_shape=jax.ShapeDtypeStruct((tgt, ex), F32),
        in_specs=[anywhere, anywhere, anywhere, vmem],
        out_specs=vmem,
        scratch_shapes=[pltpu.VMEM(*one) for one in scratch]
        + [
            pltpu.SemaphoreType.DMA((10,)),
            pltpu.SemaphoreType.DMA((112,)),
            pltpu.SemaphoreType.DMA((112,)),
        ],
        compiler_params=pltpu.CompilerParams(
            collective_id=0, has_side_effects=True, vmem_limit_bytes=63 * 2**20
        ),
    )(ex_grads, tgt_grads, projection, example_weight.reshape(1, ex))


def solution(mesh):
    placed = (P("dp", "param"), P("dp", "param"), P("param", None), P("param"))
    return jax.shard_map(
        on_device, mesh=mesh, in_specs=placed, out_specs=P("dp", "param"), check_vma=False
    )
```

```python
import functools
import math

import jax
import jax.numpy as jnp
from jax import lax
from jax.experimental import pallas as pl
from jax.experimental.pallas import tpu as pltpu
from jax.sharding import PartitionSpec as P

ridge_value = 0.5
BLK = 128
SUB = 16
TILES = 5
LATE_SUM = 7
F32, BF16 = jnp.float32, jnp.bfloat16


def tile_place(t):
    row, first = 0, 0
    for q in range(1, 12):
        past = (t + 80 - (12 * q - q * (q - 1) // 2)) // 80
        row = row + past
        first = first + past * (13 - q)
    return row, row + t - first


def tile_owner(t):
    rank, slot = divmod(t, TILES)
    half, rest = divmod(rank, 8)
    return rest // 4, half * 4 + rest % 4, slot


TILE_AT = {tile_place(t): t for t in range(78)}


def split(x):
    hi = x.astype(BF16)
    return hi, (x - hi.astype(F32)).astype(BF16)


def dot(a, b, ca, cb):
    return lax.dot_general(a, b, (((ca,), (cb,)), ((), ())), preferred_element_type=F32)


def dot3(ah, al, bh, bl, ca, cb):
    return dot(ah, bh, ca, cb) + (dot(ah, bl, ca, cb) + dot(al, bh, ca, cb))


def factor_block(d_ref):
    rows = lax.broadcasted_iota(jnp.int32, (SUB, BLK), 0)
    subs = BLK // SUB
    own = d_ref[:SUB, :]
    for s in range(subs):
        top = s * SUB
        left, right = own[:, :BLK], own[:, BLK:]
        cols = [jnp.broadcast_to(left[:, top + j : top + j + 1], (SUB, BLK)) for j in range(SUB)]
        lowers, scales, row_ls, row_rs = [], [], [], []
        for j in range(SUB):
            scale = lax.rsqrt(cols[j][j : j + 1, :])
            lower = jnp.where(rows > j, cols[j] * scale, 0.0)
            row_l = left[j : j + 1, :] * scale
            row_r = right[j : j + 1, :] * scale
            left = jnp.where(rows == j, row_l, left - lower * row_l)
            right = jnp.where(rows == j, row_r, right - lower * row_r)
            for k in range(j + 1, SUB):
                cols[k] = cols[k] - lower * lower[k : k + 1, :]
            lowers.append(lower)
            scales.append(scale)
            row_ls.append(row_l)
            row_rs.append(row_r)
        if s + 1 < subs:
            nxt = d_ref[top + SUB : top + 2 * SUB, :]
            next_l, next_r = nxt[:, :BLK], nxt[:, BLK:]
            below = [jnp.broadcast_to(next_l[:, top + j : top + j + 1], (SUB, BLK)) for j in range(SUB)]
            for j in range(SUB):
                lower = below[j] * scales[j]
                next_l = next_l - lower * row_ls[j]
                next_r = next_r - lower * row_rs[j]
                for k in range(j + 1, SUB):
                    below[k] = below[k] - lower * lowers[j][k : k + 1, :]
            own = jnp.concatenate([next_l, next_r], axis=1)
        both = jnp.concatenate([left, right], axis=1)
        d_ref[top : top + SUB, :] = both
        if s + 2 < subs:
            hi, lo = split(both)
            lhs = jnp.concatenate([hi[:, :BLK], lo[:, :BLK], hi[:, :BLK]], axis=0)
            rhs = jnp.concatenate([hi, hi, lo], axis=0)
            update = dot(lhs, rhs, 0, 0)
            d_ref[top + 2 * SUB :, :] = d_ref[top + 2 * SUB :, :] - update[top + 2 * SUB :, :]


def scores_kernel(
    inverse, out_scale, ex_ref, tgt_ref, proj_ref, w_ref, o_ref,
    stack, pv, ep, er, eg, tp, tr, tg, fall, tfeat, kp, kr, kg, g, cp, cr, cg,
    uh, ul, row, diag, ih, il, yh, yl, xh, xl, xo, og, load, send, recv,
):
    d, p = lax.axis_index("dp"), lax.axis_index("param")
    x_hi, z = d // 8, d % 8
    y, x_lo, core = p // 4, (p // 2) % 2, p % 2
    x = x_hi * 2 + x_lo
    way = 1 - 2 * core
    chip = p // 2
    pair = (d, p + way)
    n, width = fall.shape
    ex = n // 16
    blocks = n // BLK

    def at(x, y, z, core):
        return ((x // 2) * 8 + z, (y * 2 + x % 2) * 2 + core)

    def turn(v, step, n):
        return (v + step + n) % n

    started = []
    later = [None]

    def act(copy, name):
        if later[0] is None:
            getattr(copy, name)()
        else:
            later[0].append((copy, name))

    def recorded(gen):
        parts = []
        for live in [True] * 16:
            later[0] = []
            live = next(gen, "end") != "end"
            parts.append(later[0])
            if not live:
                break
        later[0] = None
        return parts

    def replay(part):
        for copy, name in part:
            getattr(copy, name)()

    def push(src, dst, device, now=True):
        i = len(started)
        copy = pltpu.make_async_remote_copy(
            src_ref=src,
            dst_ref=dst,
            send_sem=send.at[i],
            recv_sem=recv.at[i],
            device_id=device,
            device_id_type=pl.DeviceIdType.MESH,
        )
        if now:
            act(copy, "start")
        started.append(copy)
        return copy

    def landed(copies):
        for copy in copies:
            act(copy, "wait_recv")

    def run(*rings):
        live = list(rings)
        while live:
            for one in list(live):
                if next(one, "end") == "end":
                    live.remove(one)

    def chips(pieces, landing, steps=(4, 5, 3, 2, 6, 1, 7), now=True):
        return [
            push(pieces.at[(chip + s) % 8], landing.at[s - 1], (d, (p + 2 * s) % 16), now) for s in steps
        ]

    def summed(pieces, landing):
        total = pieces[chip]
        for s in range(7):
            total = total + landing[s]
        return total

    barrier = pltpu.get_barrier_semaphore()
    peers = [at(x, y, (z + s) % 8, core) for s in range(1, 8)]
    peers += [(d, (p + s) % 16) for s in range(1, 16)]
    peers += [at(turn(x, 2 * x_lo - 1, 4), y, z, core), at(turn(x, 2, 4), y, z, core)]
    for peer in peers:
        pl.semaphore_signal(barrier, inc=1, device_id=peer, device_id_type=pl.DeviceIdType.MESH)

    loads = [
        pltpu.make_async_copy(ex_ref, stack.at[:ex], load.at[8]),
        pltpu.make_async_copy(tgt_ref, stack.at[ex:], load.at[9]),
    ]
    for j in range(8):
        span = pl.ds(2 * j * width, 2 * width)
        loads.append(pltpu.make_async_copy(proj_ref.at[:, span], pv.at[j], load.at[j]))
    for copy in loads:
        copy.start()
    loads[0].wait()
    loads[1].wait()
    for j in range(8):
        loads[2 + j].wait()
        part = dot(stack[...], pv[j], 1, 0)
        for c in range(2):
            ep[c, j] = part[:ex, c * width : (c + 1) * width]
            tp[c, j] = part[ex:, c * width : (c + 1) * width]
    pl.semaphore_wait(barrier, len(peers))

    e_pair = push(ep.at[1 - core], er, pair)
    landed([e_pair])
    er[...] = er[...] + ep[core]
    e_parts = chips(er, eg)
    t_pair = push(tp.at[1 - core], tr, pair)
    landed([t_pair])
    tr[...] = tr[...] + tp[core]
    landed(e_parts)
    mine = pl.ds(pl.multiple_of(d * ex, ex), ex)
    fall[mine, :] = summed(er, eg).astype(BF16)

    def feat_rows(hi, zz):
        return fall.at[pl.ds(pl.multiple_of((hi * 8 + zz) * ex, ex), ex), :]

    other = (x_hi + 1) % 2

    ref = feat_rows(x_hi, z)
    far = push(ref, ref, at(turn(x, 2, 4), y, z, core))
    t_parts = chips(tr, tg, (3, 5))

    def along_z(hi):
        own = feat_rows(hi, z)
        near = [push(own, own, at(x, y, turn(z, step, 8), core)) for step in (2, -2, 1, -1)]
        yield
        landed(near)
        back = [feat_rows(hi, turn(z, -2, 8)), feat_rows(hi, turn(z, 2, 8))]
        away = feat_rows(hi, (z - 2 * way + 8) % 8)
        near = [
            push(away, away, at(x, y, (z + 2 * way + 8) % 8, core)),
            push(back[0], back[0], at(x, y, turn(z, 1, 8), core)),
            push(back[1], back[1], at(x, y, turn(z, -1, 8), core)),
        ]
        yield
        landed(near)
        yield

    def far_z():
        far.wait_recv()
        yield from along_z(other)

    run(along_z(x_hi), far_z())

    for i in range(TILES):
        r, c = tile_place(((z // 4 * 8 + x_hi * 4 + z % 4) * TILES + i) % 78)
        a = fall[pl.ds(pl.multiple_of(r * BLK, BLK), BLK), :]
        b = fall[pl.ds(pl.multiple_of(c * BLK, BLK), BLK), :]
        kp[:, :, i] = dot(a, b, 1, 1).reshape(8, 2, 8, BLK)
    k_pair = push(kp.at[:, 1 - core], kr, pair)
    landed([k_pair])
    kr[...] = kr[...] + kp[:, core]
    landed(chips(kr, kg))
    g[x, y, z, core] = summed(kr, kg)

    own = g.at[x, y, z, core]
    landed([push(own, own, at(x, y, (z + s) % 8, core)) for s in (4, 3, 5, 2, 6, 1, 7)])

    def gather(base):
        one, two = pl.ds(base, 2), pl.ds(base + 2, 2)

        def to_x(xx):
            return at(xx, y, z, core)

        def to_y(yy):
            return at(x, yy, z, core)

        def last_y(yy):
            return g.at[:, yy, one, core]

        def last_x(xx):
            return g.at[xx, :, two, core]

        shared = []

        def pass_on(ref):
            shared.append(push(ref, ref, pair))

        def to_all(pos, block, device):
            ref = block(pos)
            return [push(ref, ref, device((pos + step) % 4)) for step in (2, 1, 3)]

        first = to_all(x, lambda xx: g.at[xx, y, one, core], to_x)
        first += to_all(y, lambda yy: g.at[x, yy, two, core], to_y)
        yield
        landed(first)
        by_y, by_x = to_all(y, last_y, to_y), to_all(x, last_x, to_x)
        pass_on(last_y(y))
        pass_on(last_x(x))
        yield
        for i, step in ((1, 3), (2, 1), (0, 2)):
            landed([by_y[i]])
            pass_on(last_y((y + step) % 4))
            landed([by_x[i]])
            pass_on(last_x((x + step) % 4))
        landed(shared)
        yield

    upper = gather(0)
    next(upper)
    rest = recorded(gather(4))
    replay(rest[0])
    for _ in upper:
        pass
    replay(rest[1])
    t_parts += chips(tr, tg, (4, 1, 7, 2, 6))

    ident = (
        lax.broadcasted_iota(jnp.int32, (BLK, BLK), 0) == lax.broadcasted_iota(jnp.int32, (BLK, BLK), 1)
    ).astype(F32)

    def late_tile(r, c):
        return r == 3 and TILE_AT[r, c] >= 8 * TILES

    def tile_rows(r, c, q):
        o_hi, o_z, i = tile_owner(TILE_AT[r, c])
        return g[o_hi * 2 + q // 2 % 2, q // 4, o_z, q % 2, i] * inverse

    c_pair = push(cp.at[:, 1 - core], cr, pair, False)
    c_parts = chips(cr, cg, now=False)

    def step(k, carry):
        @pl.when(k == LATE_SUM)
        def _():
            landed(t_parts)
            tfeat[...] = summed(tr, tg).astype(BF16)
            cp[...] = dot(tfeat[...], fall[...], 1, 1).reshape(cp.shape)
            c_pair.start()

        @pl.when(k == LATE_SUM + 1)
        def _():
            landed([c_pair])
            cr[...] = cr[...] + cp[:, core]
            for copy in c_parts:
                copy.start()

        for kk in range(blocks):
            first = kk * BLK

            @pl.when(k == kk)
            def _(kk=kk, first=first):
                for cc in range(kk, blocks):
                    span = slice(cc * BLK, (cc + 1) * BLK)
                    if late_tile(kk, cc):
                        row[:, span] = jnp.zeros((BLK, BLK), F32)
                        continue
                    for q in range(BLK // 8):
                        row[8 * q : 8 * q + 8, span] = tile_rows(kk, cc, q)
                if kk:
                    upd = dot3(
                        uh[:first, first : first + BLK],
                        ul[:first, first : first + BLK],
                        uh[:first, first:],
                        ul[:first, first:],
                        0,
                        0,
                    )
                    row[:, first:] = row[:, first:] - upd
                diag[:, :BLK] = row[:, first : first + BLK] + ridge_value * ident

        diag[:, BLK:] = ident
        factor_block(diag)

        @pl.when(k == 3)
        def _():
            replay(rest[2])

        inv_h, inv_l = split(diag[:, BLK:])
        place = pl.ds(pl.multiple_of(k * BLK, BLK), BLK)
        ih[place, :] = inv_h
        il[place, :] = inv_l
        for kk in range(blocks - 1):
            last = (kk + 1) * BLK

            @pl.when(k == kk)
            def _(kk=kk, last=last):
                for cc in range(kk, blocks):
                    span = slice(cc * BLK, (cc + 1) * BLK)
                    if late_tile(kk, cc):
                        for q in range(BLK // 8):
                            row[8 * q : 8 * q + 8, span] += tile_rows(kk, cc, q)
                a_h, a_l = split(row[:, last:])
                u_h, u_l = split(dot3(inv_h, inv_l, a_h, a_l, 1, 0))
                uh[last - BLK : last, last:] = u_h
                ul[last - BLK : last, last:] = u_l

        return carry

    lax.fori_loop(0, blocks, step, 0)

    landed(c_parts)
    cross = summed(cr, cg) * inverse

    def against(vh, vl, mh, ml, cm):
        both = dot(jnp.concatenate([vh, vl], axis=0), mh, 1, cm)
        half = vh.shape[0]
        return both[:half] + (both[half:] + dot(vh, ml, 1, cm))

    for kk in range(blocks):
        first, last = kk * BLK, (kk + 1) * BLK
        v = cross[:, first:last]
        if kk:
            v = v - against(yh[:, :first], yl[:, :first], uh[:first, first:last], ul[:first, first:last], 0)
        v_h, v_l = split(v)
        v = against(v_h, v_l, ih[first:last, :], il[first:last, :], 1)
        v_h, v_l = split(v)
        yh[:, first:last] = v_h
        yl[:, first:last] = v_l
    for kk in reversed(range(blocks)):
        first, last = kk * BLK, (kk + 1) * BLK
        v = yh[:, first:last].astype(F32) + yl[:, first:last].astype(F32)
        if kk < blocks - 1:
            v = v - against(xh[:, last:], xl[:, last:], uh[first:last, last:], ul[first:last, last:], 1)
        v_h, v_l = split(v)
        v = against(v_h, v_l, ih[first:last, :], il[first:last, :], 0)
        v_h, v_l = split(v)
        xh[:, first:last] = v_h
        xl[:, first:last] = v_l
        row[:16, first:last] = v

    for q in range(16):
        xo[q, :, :ex] = row[:16, q * ex : (q + 1) * ex]
    finals = [push(xo.at[(p + s) % 16], og.at[s - 1], (d, (p + s) % 16)) for s in range(1, 16)]
    weight = w_ref[...] * out_scale
    o_ref[pl.ds(pl.multiple_of(p * 16, 16), 16), :] = xo[p][:, :ex] * weight
    for s in range(1, 16):
        finals[s - 1].wait_recv()
        o_ref[pl.ds(pl.multiple_of((p + 16 - s) % 16 * 16, 16), 16), :] = og[s - 1][:, :ex] * weight
    for copy in started:
        copy.wait_send()


def on_device(ex_grads, tgt_grads, projection, example_weight):
    ex, depth = ex_grads.shape
    tgt = tgt_grads.shape[0]
    columns = projection.shape[1]
    n, width, rhs = 16 * ex, columns // 16, tgt // 16
    vmem, anywhere = pl.BlockSpec(memory_space=pltpu.VMEM), pl.BlockSpec(memory_space=pl.ANY)
    scratch = [
        ((ex + tgt, depth), BF16),
        ((8, depth, 2 * width), BF16),
        ((2, 8, ex, width), F32),
        ((8, ex, width), F32),
        ((7, ex, width), F32),
        ((2, 8, tgt, width), F32),
        ((8, tgt, width), F32),
        ((7, tgt, width), F32),
        ((n, width), BF16),
        ((tgt, width), BF16),
        ((8, 2, TILES, 8, BLK), F32),
        ((8, TILES, 8, BLK), F32),
        ((7, TILES, 8, BLK), F32),
        ((4, 4, 8, 2, TILES, 8, BLK), F32),
        ((8, 2, rhs, n), F32),
        ((8, rhs, n), F32),
        ((7, rhs, n), F32),
        ((n, n), BF16),
        ((n, n), BF16),
        ((BLK, n), F32),
        ((BLK, 2 * BLK), F32),
        ((n, BLK), BF16),
        ((n, BLK), BF16),
        ((rhs, n), BF16),
        ((rhs, n), BF16),
        ((rhs, n), BF16),
        ((rhs, n), BF16),
        ((16, rhs, BLK), F32),
        ((15, rhs, BLK), F32),
    ]
    return pl.pallas_call(
        functools.partial(scores_kernel, 1.0 / columns, math.sqrt(columns)),
        out_shape=jax.ShapeDtypeStruct((tgt, ex), F32),
        in_specs=[anywhere, anywhere, anywhere, vmem],
        out_specs=vmem,
        scratch_shapes=[pltpu.VMEM(*one) for one in scratch]
        + [
            pltpu.SemaphoreType.DMA((10,)),
            pltpu.SemaphoreType.DMA((112,)),
            pltpu.SemaphoreType.DMA((112,)),
        ],
        compiler_params=pltpu.CompilerParams(
            collective_id=0, has_side_effects=True, vmem_limit_bytes=63 * 2**20
        ),
    )(ex_grads, tgt_grads, projection, example_weight.reshape(1, ex))


def solution(mesh):
    placed = (P("dp", "param"), P("dp", "param"), P("param", None), P("param"))
    return jax.shard_map(
        on_device, mesh=mesh, in_specs=placed, out_specs=P("dp", "param"), check_vma=False
    )
```
